32 devices in a mesh: dp: 1 (over z), tp: 4 (over y), cp: 8 (over x, core).
Axes of the slice: x: 4, y: 4, z: 1, core: 2. Of those that a mesh axis runs over, the one named last changes fastest.
The devices are a block of a 4x4x8 slice.
Arguments:
- hidden: bfloat16 [8192, 3840], P(('dp', 'cp'))
- positions: int32 [8192], P(('dp', 'cp'))
- w_q: bfloat16 [2, 3840, 4096], P(None, None, 'tp')
- w_k: bfloat16 [2, 3840, 2048], P(None, None, 'tp')
- w_v: bfloat16 [2, 3840, 2048], P(None, None, 'tp')
- w_o: bfloat16 [2, 4096, 3840], P(None, 'tp')
- w_gate: bfloat16 [2, 3840, 15360], P(None, None, 'tp')
- w_up: bfloat16 [2, 3840, 15360], P(None, None, 'tp')
- w_down: bfloat16 [2, 15360, 3840], P(None, 'tp')
- norm_gain: float32 [2, 4, 3840], replicated
- qk_gain: float32 [2, 2, 256], replicated
Outputs:
- output 1: bfloat16 [8192, 3840], P(('dp', 'cp'))
- output 2: bfloat16 [2, 8192, 8, 256], P(None, ('dp', 'cp'), 'tp')
- output 3: bfloat16 [2, 8192, 8, 256], P(None, ('dp', 'cp'), 'tp')
All inputs are finite; a program needn't handle non-finite values.
Results may differ from the reference program's by a relative error of at most 0.0164515.
Values are sent between devices in bfloat16 or wider.
A program may use at most 768 MiB of HBM per device.

```python
import jax
import jax.numpy as jnp
from jax import lax

D = 3840
HEADS = 16
KV_HEADS = 8
HEAD = 256
FF = 15360
WINDOW = 1024
TOKENS = 8192

EPS = 1e-6
THETAS = (10000.0, 1000000.0)
LAYER_WINDOWS = (WINDOW, TOKENS)
Q_BLOCK = min(32, TOKENS)


def normal_weight(key_in, arr_shape, fan_in):
    scale_val = fan_in ** -0.5
    return (jax.random.normal(key_in, arr_shape, jnp.float32) * scale_val).astype(jnp.bfloat16)


def setup_inputs(seed: int = 0, part: int = 0) -> dict:
    part_key = jax.random.fold_in(jax.random.key(seed), part)
    key_hidden, key_start = jax.random.split(part_key, 2)
    shared = jax.random.split(jax.random.key(seed + 1), 9)
    hidden = jax.random.normal(key_hidden, (TOKENS, D), jnp.float32).astype(jnp.bfloat16)
    start_pos = jax.random.randint(key_start, (), 0, 1024)
    positions = (start_pos + jnp.arange(TOKENS)).astype(jnp.int32)
    return {
        'hidden': hidden,
        'positions': positions,
        'w_q': normal_weight(shared[0], (2, D, HEADS * HEAD), D),
        'w_k': normal_weight(shared[1], (2, D, KV_HEADS * HEAD), D),
        'w_v': normal_weight(shared[2], (2, D, KV_HEADS * HEAD), D),
        'w_o': normal_weight(shared[3], (2, HEADS * HEAD, D), HEADS * HEAD),
        'w_gate': normal_weight(shared[4], (2, D, FF), D),
        'w_up': normal_weight(shared[5], (2, D, FF), D),
        'w_down': normal_weight(shared[6], (2, FF, D), FF),
        'norm_gain': 0.4 * jax.random.normal(shared[7], (2, 4, D), jnp.float32),
        'qk_gain': 0.4 * jax.random.normal(shared[8], (2, 2, HEAD), jnp.float32),
    }


def rms_scale(values, gain):
    mean_sq = jnp.mean(values * values, axis=-1, keepdims=True)
    return values * lax.rsqrt(mean_sq + EPS) * (1.0 + gain)


def rotary(values, positions, theta):
    half_dim = HEAD // 2
    inv_freq = theta ** (-(jnp.arange(half_dim, dtype=jnp.float32) * 2.0) / HEAD)
    angles = positions.astype(jnp.float32)[..., None] * inv_freq
    cosine = jnp.cos(angles)[..., None, :]
    sine_val = jnp.sin(angles)[..., None, :]
    lower_half = values[..., :half_dim]
    upper_half = values[..., half_dim:]
    return jnp.concatenate([lower_half * cosine - upper_half * sine_val, upper_half * cosine + lower_half * sine_val], axis=-1)


def attention(queries, key_rows, val_rows, window):
    groups = HEADS // KV_HEADS
    score_scale = HEAD ** -0.5
    key_f = key_rows.astype(jnp.float32)
    val_f = val_rows.astype(jnp.float32)
    q_blocks = queries.reshape(TOKENS // Q_BLOCK, Q_BLOCK, KV_HEADS, groups, HEAD)
    key_index = jnp.arange(TOKENS)

    def one_block(block_args):
        q_block, block_id = block_args
        scores = jnp.einsum('qhgd,uhd->hgqu', q_block.astype(jnp.float32), key_f) * score_scale
        query_index = block_id * Q_BLOCK + jnp.arange(Q_BLOCK)
        distance = query_index[:, None] - key_index[None, :]
        allowed = (distance >= 0) & (distance < window)
        scores = jnp.where(allowed, scores, -jnp.inf)
        prob_all = jax.nn.softmax(scores, axis=-1)
        return jnp.einsum('hgqu,uhd->qhgd', prob_all, val_f)

    block_out = lax.map(one_block, (q_blocks, jnp.arange(TOKENS // Q_BLOCK)))
    return block_out.reshape(TOKENS, HEADS * HEAD).astype(jnp.bfloat16)


def reference(hidden, positions, w_q, w_k, w_v, w_o, w_gate, w_up, w_down, norm_gain, qk_gain):
    state_f = hidden.astype(jnp.float32)
    new_hidden = hidden
    k_list = []
    v_list = []
    for layer_id in range(2):
        layer_gain = norm_gain[layer_id]
        normed = rms_scale(state_f, layer_gain[0]).astype(jnp.bfloat16)
        q_proj = jnp.dot(normed, w_q[layer_id], preferred_element_type=jnp.float32).reshape(TOKENS, HEADS, HEAD)
        k_proj = jnp.dot(normed, w_k[layer_id], preferred_element_type=jnp.float32).reshape(TOKENS, KV_HEADS, HEAD)
        v_rows = jnp.dot(normed, w_v[layer_id], preferred_element_type=jnp.float32).astype(jnp.bfloat16).reshape(TOKENS, KV_HEADS, HEAD)
        q_rot = rotary(rms_scale(q_proj, qk_gain[layer_id, 0]), positions, THETAS[layer_id]).astype(jnp.bfloat16)
        k_rot = rotary(rms_scale(k_proj, qk_gain[layer_id, 1]), positions, THETAS[layer_id]).astype(jnp.bfloat16)
        attn_rows = attention(q_rot, k_rot, v_rows, LAYER_WINDOWS[layer_id])
        attn_out = jnp.dot(attn_rows, w_o[layer_id], preferred_element_type=jnp.float32)
        resid_f = (state_f + rms_scale(attn_out, layer_gain[1])).astype(jnp.bfloat16).astype(jnp.float32)
        normed_mlp = rms_scale(resid_f, layer_gain[2]).astype(jnp.bfloat16)
        gate_proj = jnp.dot(normed_mlp, w_gate[layer_id], preferred_element_type=jnp.float32)
        up_proj = jnp.dot(normed_mlp, w_up[layer_id], preferred_element_type=jnp.float32)
        act_rows = (jax.nn.gelu(gate_proj, approximate=True) * up_proj).astype(jnp.bfloat16)
        mlp_out = jnp.dot(act_rows, w_down[layer_id], preferred_element_type=jnp.float32)
        new_hidden = (resid_f + rms_scale(mlp_out, layer_gain[3])).astype(jnp.bfloat16)
        state_f = new_hidden.astype(jnp.float32)
        k_list.append(k_rot)
        v_list.append(v_rows)
    return new_hidden, jnp.stack(k_list), jnp.stack(v_list)
```

```python
import functools
import jax
import jax.numpy as jnp
from jax import lax
from jax.experimental import pallas as pl
from jax.experimental.pallas import tpu as pltpu
from jax.sharding import PartitionSpec as P

WINDOW = 1024
THETAS = (10000.0, 1000000.0)
EPS = 1e-6
NEG_BIG = -1e30
BF = jnp.bfloat16
F32 = jnp.float32
MESH = pl.DeviceIdType.MESH
ANY = pl.BlockSpec(memory_space=pl.ANY)
LOG2E = 1.4426950408889634
PAIR = 2
TWO = (0, 1)
TRIO = (0, 1, 2)
TILE = 256
LANES = 128
BIG_VMEM = 67_000_000
DMA = pltpu.SemaphoreType.DMA
VM = pltpu.VMEM


def span(start, size, unit=16):
    return pl.ds(pl.multiple_of(start, unit), size)


def send(src, dst, sent, received, to):
    return pltpu.make_async_remote_copy(src_ref=src, dst_ref=dst, send_sem=sent, recv_sem=received, device_id=to, device_id_type=MESH)


def each(method, *groups):
    for group in groups:
        for item in group:
            getattr(item, method)()


def start(*groups):
    each('start', *groups)


def wait(*groups):
    each('wait', *groups)


def arrived(*groups):
    each('wait_recv', *groups)


def departed(*groups):
    each('wait_send', *groups)


def greet(peers):
    barrier = pltpu.get_barrier_semaphore()
    for to in peers:
        pl.semaphore_signal(barrier, inc=1, device_id=to, device_id_type=MESH)
    pl.semaphore_wait(barrier, len(peers))


def around(axis, n, *distances):
    return [lax.rem(lax.axis_index(axis) + n + d, n) for d in distances]


def tp_peers(n_tp):
    return around('tp', n_tp, 1, -1, PAIR)


def cp_peers(n_cp):
    cp = lax.axis_index('cp')
    return (*around('cp', n_cp, PAIR, -PAIR, PAIR * PAIR), cp + 1 - PAIR * lax.rem(cp, PAIR))


def head_of(size):
    return pl.ds(0, size)


def on(axis, *devices):
    return [{axis: dev} for dev in devices]


def mean_scale(values):
    return lax.rsqrt(jnp.mean(values * values, axis=-1, keepdims=True) + EPS)


def rotate_heads(values, gain, cosine, sine):
    half = cosine.shape[-1]
    normed = values * mean_scale(values) * gain
    lower, upper = normed[:, :half], normed[:, half:]
    return jnp.concatenate([lower * cosine - upper * sine, upper * cosine + lower * sine], axis=-1).astype(BF)


def first_kernel(
    n_q, n_kv, n_tp, n_cp, strip, cut,
    x_ref, wk_ref, wv_ref, wq_ref, gain_ref, qg_ref, kg_ref, cos_ref, sin_ref, wo_hbm,
    o_hbm, kc_hbm, vc_hbm, wo_all, wo_next,
    h_ref, q_ref, kv_ref, past_ref,
    y1s, y1r, y2s, y2r, x1s, x1r, x2s, x2r, rs, rr, ks, kr, csem, osem,
):
    step = pl.program_id(0)
    rows = x_ref.shape[0]
    dim = qg_ref.shape[-1]
    o_rows = wo_hbm.shape[1]
    n_x = n_cp // PAIR
    shared = (o_rows // PAIR - n_x * strip) // PAIR

    me, cp = lax.axis_index('tp'), lax.axis_index('cp')
    core, chip = lax.rem(cp, PAIR), cp // PAIR
    right, left, opposite = tp_peers(n_tp)
    sides, sources = on('tp', right, left), (left, right, opposite)
    *ends, _, partner = on('cp', *cp_peers(n_cp))
    follow, prior = on('cp', *around('cp', n_cp, 1, -1))
    base = core * (o_rows // PAIR)

    def strip_of(distance):
        return base + PAIR * shared + lax.rem(chip + n_x + distance, n_x) * strip

    piece = o_rows // n_cp
    pieces = ((strip_of(0), strip, cut), (base, shared, shared // PAIR), (base + shared, shared, shared // PAIR), (cp * piece, piece, piece // PAIR))
    final = len(pieces) - 1

    def target(p):
        return wo_next if p == final else wo_all

    def y_first(p):
        at = span(*pieces[p][:PAIR])
        return [send(wo_hbm.at[p // final, at, :], target(p).at[me, at, :], y1s.at[p, d], y1r.at[p, d], sides[d]) for d in TWO]

    def halves(first, size, cut):
        return span(first, cut), span(first + cut, size - cut)

    def y_second(p):
        refs = [target(p).at[sources[d], halves(*pieces[p])[d], :] for d in TWO]
        return [send(refs[d], refs[d], y2s.at[p, d], y2r.at[p, d], sides[d]) for d in TWO]

    def x_first(s):
        ref = wo_all.at[sources[s], span(strip_of(0), strip), :]
        return [send(ref, ref, x1s.at[s, d], x1r.at[s, d], ends[d]) for d in TWO]

    def x_second(s):
        refs = [wo_all.at[sources[s], halves(strip_of((-1, 1)[d]), strip, cut)[d], :] for d in TWO]
        return [send(refs[d], refs[d], x2s.at[s, d], x2r.at[s, d], ends[d]) for d in TWO]

    def relay(kind, s):
        first, size = pieces[kind][:PAIR] if kind < final else (strip_of(kind - PAIR), strip)
        ref = wo_all.at[sources[s], span(first, size), :]
        return [send(ref, ref, rs.at[kind, s], rr.at[kind, s], partner)]

    def send_kv(t):
        return [send(kv_ref.at[t], past_ref.at[t], ks.at[t], kr.at[t], follow)]

    def keep_kv(t):
        return [pltpu.make_async_copy(kv_ref.at[t], (kc_hbm, vc_hbm)[t].at[0], csem.at[t])]

    group = n_q // n_kv

    def keep_o(h):
        some = pl.ds(h * group * dim, group * dim)
        return [pltpu.make_async_copy(q_ref.at[:, some], o_hbm.at[:, some], osem.at[h])]

    def y_stage(p, *more):
        arrived(y_first(p))
        start(y_second(p), *more, *[relay(p, s) for s in TWO if p < final])

    def x_stage(s):
        arrived(x_first(s))
        start(x_second(s), relay(final, s), relay(final + PAIR, s))

    def y_end(p):
        arrived(y_second(p))
        start(relay(p, PAIR), *([] if p else [x_first(PAIR)]))

    def x_end(s):
        arrived(x_second(s))
        start(relay(final + 1, s))

    q_step = PAIR * n_kv

    @pl.when(step == 0)
    def _():
        greet((*sides, *ends, follow, prior))
        start(*map(y_first, TWO))
        rb = 32

        @pl.loop(0, rows // rb)
        def _(i):
            at = span(i * rb, rb)
            xf = x_ref[at, :].astype(F32)
            h_ref[at, :] = (xf * mean_scale(xf) * gain_ref[...]).astype(BF)

    @pl.when(step == n_kv)
    def _():
        start(send_kv(0), keep_kv(0))

    @pl.when(step == q_step)
    def _():
        start(send_kv(1), keep_kv(1))
        y_stage(0, y_first(PAIR), *map(x_first, TWO))

    @pl.when(step == q_step + 3)
    def _():
        x_stage(0)

    def project(w_ref, store, finish):
        @pl.loop(0, rows // TILE)
        def _(i):
            at = span(i * TILE, TILE)
            store(at, finish(jnp.dot(h_ref[at, :], w_ref[0], preferred_element_type=F32), at))

    def into_kv(t, head):
        def store(at, value):
            kv_ref[t, at, span(head * dim, dim, LANES)] = value
        return store

    def into_q(at, value):
        q_ref[at, span((step - q_step) * dim, dim, LANES)] = value

    def rotate(gain_ref):
        return lambda a, at: rotate_heads(a, gain_ref[...], cos_ref[at, :], sin_ref[at, :])

    @pl.when(step < n_kv)
    def _():
        project(wk_ref, into_kv(0, step), rotate(kg_ref))

    @pl.when((step >= n_kv) & (step < q_step))
    def _():
        project(wv_ref, into_kv(1, step - n_kv), lambda a, at: a.astype(BF))

    @pl.when(step >= q_step)
    def _():
        project(wq_ref, into_q, rotate(qg_ref))

    def attend(h):
        head = slice(h * dim, (h + 1) * dim)
        for g in range(group):
            local_head(q_ref, h * group + g, *[ref.at[t, :, head] for t in TWO for ref in (past_ref, kv_ref)])
        start(keep_o(h))

    @pl.when(step == q_step + n_q - 1)
    def _():
        y_stage(1, y_first(final))
        y_end(0)
        x_stage(1)
        arrived(*map(send_kv, TWO))
        attend(0)
        x_end(0)
        y_stage(PAIR)
        x_stage(PAIR)
        y_stage(final)
        for h in range(1, n_kv):
            attend(h)
        x_end(1)
        y_end(1)
        y_end(PAIR)
        x_end(PAIR)
        arrived(y_second(final))
        departed(*map(send_kv, TWO))
        wait(*map(keep_kv, TWO), *map(keep_o, range(n_kv)))
        for s in TRIO:
            wait(*[relay(kind, s) for kind in range(PAIR * len(TRIO))])
            departed(x_first(s), x_second(s))
        for p in range(len(pieces)):
            departed(y_first(p), y_second(p))


def first_call(n_tp, n_cp, x, w_q, w_k, w_v, w_o, gain, q_gain, k_gain, cosine, sine):
    rows, width = x.shape
    dim = q_gain.shape[-1]
    n_q, n_kv = w_q.shape[-1] // dim, w_k.shape[-1] // dim
    at_k = lambda t: jnp.minimum(t, n_kv - 1)
    at_v = lambda t: jnp.clip(t - n_kv, 0, n_kv - 1)
    at_q = lambda t: jnp.maximum(t - PAIR * n_kv, 0)
    whole = lambda a: pl.BlockSpec(a.shape, lambda t: TWO[:1] * PAIR, pipeline_mode=pl.Buffered(1))
    w_spec = lambda at: pl.BlockSpec((1, width, dim), lambda t: (0, 0, at(t)))
    shape = lambda *sizes: jax.ShapeDtypeStruct(sizes, BF)
    q_width, kv_width = n_q * dim, n_kv * dim
    work = PAIR * width * (q_width + PAIR * kv_width)
    gathered, cache = shape(n_tp, *w_o.shape[1:]), shape(PAIR, rows, kv_width)
    return pl.pallas_call(
        functools.partial(first_kernel, n_q, n_kv, n_tp, n_cp, 80, 48),
        grid=(n_q + PAIR * n_kv,),
        in_specs=[whole(x), *map(w_spec, (at_k, at_v, at_q)), *map(whole, (gain, q_gain, k_gain, cosine, sine)), ANY],
        out_specs=[ANY] * 5,
        out_shape=[shape(rows, q_width), cache, cache, gathered, gathered],
        scratch_shapes=[VM((rows, width), BF), VM((rows, q_width), BF), VM(cache.shape, BF), VM(cache.shape, BF)]
        + [DMA((4, PAIR))] * 8 + [DMA((6, 3))] * PAIR + [DMA((PAIR,))] * 3 + [DMA((n_kv,))],
        compiler_params=pltpu.CompilerParams(dimension_semantics=("arbitrary",), collective_id=2, has_side_effects=True, vmem_limit_bytes=BIG_VMEM),
        cost_estimate=pl.CostEstimate(flops=rows * work, bytes_accessed=work, transcendentals=0),
        name="first",
    )(x, w_k, w_v, w_q, gain, q_gain, k_gain, cosine, sine, w_o)


def scores_of(q, k):
    return lax.dot_general(q, k, (((1,), (1,)), ((), ())), preferred_element_type=F32)


def local_head(q_ref, head, kp_ref, ko_ref, vp_ref, vo_ref):
    rows, dim = ko_ref.shape
    tile = TILE
    scale = dim ** -0.5 * LOG2E
    opening = lax.axis_index('cp') == 0
    row = lax.broadcasted_iota(jnp.int32, (tile, tile), 0)
    col = lax.broadcasted_iota(jnp.int32, (tile, tile), 1)
    for begin in range(0, rows, tile):
        end = begin + tile
        at = (slice(begin, end), slice(head * dim, (head + 1) * dim))
        q = q_ref[at]
        past = scores_of(q, kp_ref[begin:, :])
        here = scores_of(q, ko_ref[:end, :])
        past = jnp.concatenate([jnp.where(col > row, past[:, :tile], NEG_BIG), past[:, tile:]][:1 + (end < rows)], axis=1)
        past = jnp.where(opening, NEG_BIG, past)
        here = jnp.concatenate([here[:, :begin], jnp.where(col <= row, here[:, begin:], NEG_BIG)][begin == 0:], axis=1)
        top = jnp.maximum(*[jnp.max(a, axis=1, keepdims=True) for a in (past, here)])
        probs = [jnp.exp2((a - top) * scale) for a in (past, here)]
        total = sum(jnp.sum(p, axis=1, keepdims=True) for p in probs)
        acc = sum(jnp.dot(p.astype(BF), v, preferred_element_type=F32) for p, v in zip(probs, (vp_ref[begin:, :], vo_ref[:end, :])))
        q_ref[at] = (acc / total).astype(BF)


def fold_rows(values, op):
    return op(values.reshape(-1, 8, values.shape[-1]), axis=0)


def row_gather(n_tp, unit, gathered, own, s1, r1, s2, r2):
    sides = on('tp', *tp_peers(n_tp)[:PAIR])
    half = gathered.shape[-1] // PAIR
    seen = TRIO[::-PAIR]

    def first(u):
        at = span(u * unit, unit)
        return [send(own.at[at, :], gathered.at[seen[d], at, :], s1.at[u, d], r1.at[u, d], sides[d]) for d in TWO]

    def second(u):
        at = span(u * unit, unit)
        cols = [slice(d * half, (d + 1) * half) for d in TWO]
        return [send(gathered.at[seen[d], at, cols[d]], gathered.at[1, at, cols[d]], s2.at[u, d], r2.at[u, d], sides[d]) for d in TWO]

    return sides, first, second


def global_kernel(
    groups, n_tp, unit, q_ref, k_hbm, vt_hbm, o_hbm, og_hbm,
    k_ref, vt_ref, o_ref, m_ref, l_ref, ka_ref, kb_ref, xa_ref, xb_ref, acc_ref, sa_ref, sb_ref, pa_ref, pb_ref,
    ksem, vsem, osem, s1, r1, s2, r2,
):
    rows, width = q_ref.shape
    dim = acc_ref.shape[0]
    n_kv = k_hbm.shape[1] // dim
    block, wide = sa_ref.shape
    tile = wide // groups
    scale = dim ** -0.5 * LOG2E
    cp = lax.axis_index('cp')
    base = cp * (rows // block)
    last = base - 1
    sides, first, second = row_gather(n_tp, unit, og_hbm, o_ref, s1, r1, s2, r2)
    ready = tile // unit

    def load(b):
        at = span(b * rows, rows, LANES)
        return [pltpu.make_async_copy(k_hbm.at[at, :], k_ref.at[at, :], ksem.at[b]), pltpu.make_async_copy(vt_hbm.at[:, at], vt_ref.at[:, at], vsem.at[b])]

    def store(i):
        at = span(i * tile, tile)
        return [pltpu.make_async_copy(o_ref.at[at, :], o_hbm.at[at, :], osem.at[i])]

    @pl.loop(0, cp + 1)
    def _(b):
        start(load(cp - b))

    greet(sides)
    wait(load(cp))

    key = lax.broadcasted_iota(jnp.int32, (block, wide), 0)
    token = lax.rem(lax.broadcasted_iota(jnp.int32, (block, wide), 1), tile)

    @pl.loop(0, n_kv * (rows // tile))
    def _(turn):
        i, h = turn // n_kv, lax.rem(turn, n_kv)
        head = span(h * dim, dim, LANES)

        @pl.when(turn == 0)
        def _():
            @pl.loop(0, cp)
            def _(b):
                wait(load(b))

        q = jnp.concatenate([q_ref[span(i * tile, tile), span((h * groups + g) * dim, dim, LANES)] for g in range(groups)], axis=0)

        def score(b, s_ref, x_ref, masked=False):
            s = scores_of(k_ref[span(b * block, block), head], q)
            if masked:
                s = jnp.where(key <= token, s, NEG_BIG)
            s_ref[...] = s
            x_ref[...] = fold_rows(s, jnp.max)

        def soften(s_ref, x_ref, p_ref, keep_ref, opening=False):
            top = jnp.max(x_ref[...], axis=0, keepdims=True)
            if not opening:
                old = m_ref[...]
                top = jnp.maximum(old, top)
                keep_ref[...] = jnp.exp2((old - top) * scale)
            m_ref[...] = top
            prob = jnp.exp2((s_ref[...] - top) * scale)
            part = fold_rows(prob, jnp.sum)
            l_ref[...] = part if opening else l_ref[...] * keep_ref[...] + part
            p_ref[...] = prob.astype(BF)

        def weigh(b, p_ref, keep_ref, opening=False):
            part = jnp.dot(vt_ref[head, span(b * block, block, LANES)], p_ref[...], preferred_element_type=F32)
            acc_ref[...] = part if opening else acc_ref[...] * keep_ref[...] + part

        score(base + i, sa_ref, xa_ref, True)
        soften(sa_ref, xa_ref, pa_ref, ka_ref, True)
        weigh(base + i, pa_ref, ka_ref, True)

        @pl.loop(0, i)
        def _(b):
            score(base + b, sa_ref, xa_ref)
            soften(sa_ref, xa_ref, pa_ref, ka_ref)
            weigh(base + b, pa_ref, ka_ref)

        @pl.when(cp > 0)
        def _():
            score(jnp.int32(0), sa_ref, xa_ref)
            pb_ref[...] = jnp.zeros_like(pb_ref)
            kb_ref[...] = jnp.ones_like(kb_ref)

            @pl.loop(0, base // PAIR)
            def _(half):
                b = PAIR * half
                score(b + 1, sb_ref, xb_ref)
                soften(sa_ref, xa_ref, pa_ref, ka_ref)
                weigh(jnp.maximum(b - 1, 0), pb_ref, kb_ref)
                score(jnp.minimum(b + PAIR, last), sa_ref, xa_ref)
                soften(sb_ref, xb_ref, pb_ref, kb_ref)
                weigh(b, pa_ref, ka_ref)

            weigh(last, pb_ref, kb_ref)

        out = (acc_ref[...] / jnp.sum(l_ref[...], axis=0, keepdims=True)).T.astype(BF)
        for g in range(groups):
            o_ref[span(i * tile, tile), span((h * groups + g) * dim, dim, LANES)] = out[g * tile:(g + 1) * tile]

        @pl.when(turn == n_kv - 1)
        def _():
            start(store(0), *map(first, range(ready)))

        @pl.when(turn == n_kv)
        def _():
            for u in range(ready - 1):
                arrived(first(u))
                start(second(u))

    start(store(1))
    arrived(first(ready - 1))
    start(second(ready - 1))
    for u in range(ready):
        departed(first(u))
        wait(second(u))
    wait(*map(store, TWO))


def global_call(n_tp, q, k_all, vt_all, dim):
    rows, width = q.shape
    every, kv_width = k_all.shape
    groups = width // kv_width
    tile = rows // PAIR
    wide = groups * tile
    unit = LANES
    vmem = pl.BlockSpec(memory_space=VM)
    row, slab = VM((1, wide), F32), VM((8, wide), F32)
    return pl.pallas_call(
        functools.partial(global_kernel, groups, n_tp, unit),
        in_specs=[vmem, ANY, ANY],
        out_specs=[ANY, ANY],
        out_shape=[jax.ShapeDtypeStruct(q.shape, BF), jax.ShapeDtypeStruct((n_tp - 1, *q.shape), BF)],
        scratch_shapes=[VM(k_all.shape, BF), VM(vt_all.shape, BF), VM(q.shape, BF), row, slab, row, row, slab, slab, VM((dim, wide), F32)]
        + [VM((tile, wide), t) for t in (F32, F32, BF, BF)] + [DMA((every // rows,))] * PAIR + [DMA((PAIR,))] + [DMA((tile // unit, PAIR))] * 4,
        compiler_params=pltpu.CompilerParams(collective_id=3, has_side_effects=True, vmem_limit_bytes=BIG_VMEM),
        cost_estimate=pl.CostEstimate(flops=PAIR * rows * every * width, bytes_accessed=PAIR * every * width, transcendentals=0),
        name="attend_global",
    )(q, k_all, vt_all)


def block_kernel(layer, n_tp, n_cp, tm, nt, unit, ready, follow, *refs):
    queue = iter(refs)

    def take(names):
        return [ref for _, ref in zip(range(names), queue)]

    o_hbm, wo_own, wo_hbm, x_hbm, wg_hbm, wu_hbm, wd_hbm, gain_ref = take(8)
    if ready:
        take(1)
    if follow:
        wq_hbm, wk_hbm, wv_hbm, hg_ref, qg_ref, kg_ref, cos_ref, sin_ref, *_ = take(11)
    out_hbm, og_hbm = take(PAIR)
    if follow:
        q_hbm, ka_hbm, va_hbm, k_hbm, v_hbm, wn_hbm = take(6)
    wbuf, pbuf, r1, r2, xb, mbuf, sbuf, obuf, xbuf, rown, wsem, osem, xsem, stsem = take(14)
    o1s, o1r, o2s, o2r, s1s, s1r, sbs, sbr, sas, sar, g1s, g1r, g2s, g2r = take(14)
    if follow:
        nbuf, vbuf, nsem, fs, fr, hs, hr, ps, pr, a1s, a1r, a2s, a2r, bs, br_ = take(15)

    rows, width = x_hbm.shape
    o_width = o_hbm.shape[1]
    hidden = wd_hbm.shape[1]
    chunks = rows // tm
    fine = tm // unit
    br = unit // n_tp
    hw = width // PAIR
    units = rows // unit
    n_o, n_g, n_d = width // nt, hidden // nt, width // nt
    n_og = n_o + PAIR * n_g
    per = n_og + n_d
    depth, lag = 3, PAIR
    n_n = 0
    if follow:
        dim = qg_ref.shape[-1]
        nw = wk_hbm.shape[-1]
        n_qt = wq_hbm.shape[-1] // nw
        n_n = n_qt + PAIR
    total = chunks * per + (chunks + 1) * n_n

    me, cp = lax.axis_index('tp'), lax.axis_index('cp')
    right, left, opposite = tp_peers(n_tp)
    near = (right, left)
    far = (left, right)
    ahead, behind, across, mate = cp_peers(n_cp)
    *ends, partner = on('cp', ahead, behind, mate)
    sides, o_first, o_second = row_gather(n_tp, unit, og_hbm, o_hbm, o1s, o1r, o2s, o2r)

    def base_of(n):
        return n * per + jnp.maximum(n - lag, 0) * n_n

    def step_of(index):
        if not follow:
            return lax.rem(index, per)
        head, body = lag * per, (chunks - lag) * (per + n_n)
        late = index - head
        tail = per + lax.rem(jnp.maximum(late - body, 0), n_n)
        return jnp.where(late < 0, lax.rem(index, per), jnp.where(late < body, lax.rem(jnp.maximum(late, 0), per + n_n), tail))

    def columns(tile):
        return span(tile * nt, nt, LANES)

    def part_of(slot, length, first=0):
        return wbuf.at[slot, pl.ds(first, length), :]

    def narrow(slot):
        return wbuf.at[slot, head_of(width), head_of(nw)]

    def start_w(index):
        step, slot = step_of(index), lax.rem(index, depth)

        def load(wanted, src, dst, s=0):
            @pl.when((index < total) & wanted)
            def _():
                pltpu.make_async_copy(src, dst, wsem.at[slot, s]).start()

        for s in range(n_tp):
            src = wo_hbm.at[lax.rem(me + s, n_tp)] if s else wo_own.at[layer]
            load(step < n_o, src.at[:, columns(jnp.minimum(step, n_o - 1))], part_of(slot, o_width, s * o_width), s)
        middle = jnp.clip(step - n_o, 0, n_og - n_o - 1)
        for t, src in enumerate((wg_hbm, wu_hbm)):
            load((step >= n_o) & (step < n_og) & (lax.rem(middle, PAIR) == t), src.at[layer, :, columns(middle // PAIR)], part_of(slot, width))
        load((step >= n_og) & (step < per), wd_hbm.at[layer, :, columns(jnp.clip(step - n_og, 0, n_d - 1))], part_of(slot, hidden))
        if follow:
            for t, src in enumerate((wk_hbm, wv_hbm)):
                load(step == per + t, src.at[layer + 1], narrow(slot))
            late = step - per - PAIR
            load(late >= 0, wq_hbm.at[layer + 1, :, span(jnp.clip(late, 0, n_qt - 1) * nw, nw, LANES)], narrow(slot))

    def wait_w(index, length):
        slot = lax.rem(index, depth)
        pltpu.make_async_copy(wd_hbm.at[layer, head_of(length), columns(0)], part_of(slot, length), wsem.at[slot, 0]).wait()
        return slot

    def wait_wo(index):
        slot = lax.rem(index, depth)
        for s in range(n_tp):
            pltpu.make_async_copy(wo_own.at[layer, :, columns(0)], part_of(slot, o_width, s * o_width), wsem.at[slot, s]).wait()
        return slot

    def o_serve(u):
        arrived(o_first(u))
        start(o_second(u))

        @pl.when(u + PAIR < units)
        def _():
            start(o_first(u + PAIR))

    def o_finish(u):
        departed(o_first(u))
        wait(o_second(u))

    cols = [pl.ds(d * hw, hw) for d in TWO]
    other = cols[::-1]

    def partial(k):
        return pbuf.at[lax.rem(k // fine, PAIR)]

    def part(k, dev):
        return span(lax.rem(k, fine) * unit + dev * br, br)

    def reduce(kind, k, d, dev, side, dst):
        s_sem, r_sem = kind
        return [send(partial(k).at[part(k, dev), side], dst, s_sem.at[k, d], r_sem.at[k, d], sides[d])]

    def s_far(k, d):
        return reduce((s1s, s1r), k, d, opposite, cols[d], r1.at[k, d])

    def s_plain(k, d):
        return reduce((sbs, sbr), k, d, near[d], other[d], r2.at[k, d, :, other[d]])

    def s_sum(k, d):
        return reduce((sas, sar), k, d, near[d], cols[d], r2.at[k, d, :, cols[d]])

    def x_rows(k, dev):
        return span(k * unit + dev * br, br)

    def x_first(k):
        return [send(xb.at[k], out_hbm.at[x_rows(k, me), :], g1s.at[k, d], g1r.at[k, d], sides[d]) for d in TWO]

    def x_second(k):
        refs = [out_hbm.at[x_rows(k, far[d]), cols[d]] for d in TWO]
        return [send(refs[d], refs[d], g2s.at[k, d], g2r.at[k, d], sides[d]) for d in TWO]

    def x_own(k):
        return [pltpu.make_async_copy(xb.at[k], out_hbm.at[x_rows(k, me), :], stsem.at[k])]

    def e0(n):
        for kind in (s_far, s_plain):
            for i in range(fine):
                start(*[kind(n * fine + i, d) for d in TWO])

    def e1(k):
        p = partial(k)
        for d in TWO:
            at = (part(k, near[d]), cols[d])
            arrived(s_far(k, d))
            p[at] = p[at] + r1[k, d]
            start(s_sum(k, d))

    def e2(k):
        p = partial(k)
        for d in TWO:
            arrived(s_plain(k, d), s_sum(k, d))
        sub = 16
        for begin in range(0, br, sub):
            at = pl.ds(begin, sub)
            z = sum([r2[k, d, at, :] for d in TWO], p[span(lax.rem(k, fine) * unit + me * br + begin, sub), :])
            r = rown[lax.rem(k // fine, PAIR), lax.rem(k, fine), at, :].astype(F32)
            xb[k, at, :] = (r + z * mean_scale(z) * gain_ref[PAIR:, :]).astype(BF)
        start(x_first(k), x_own(k))
        for d in TWO:
            departed(s_far(k, d), s_plain(k, d), s_sum(k, d))

    def e3(k):
        arrived(x_first(k))
        start(x_second(k))

    def e4(k):
        wait(x_second(k), x_own(k))
        departed(x_first(k))

    def all_of(step, n):
        for i in range(fine):
            step(n * fine + i)

    def batch(n):
        return n, n * tm, tm

    ends_of = [(jnp.int32(chunks - 1 + i), jnp.int32(rows - tm + i * unit), unit) for i in TWO]

    def kv_at(c, dev, t):
        at = span(dev * rows + c[1], c[PAIR], LANES)
        return va_hbm.at[:, at] if t else ka_hbm.at[at, :]

    def kv_mine(c, t):
        slot, some = lax.rem(c[0], depth), head_of(c[PAIR])
        return vbuf.at[slot, :, some] if t else nbuf.at[slot, 0, some, :]

    def kv_first(c):
        return [send(kv_mine(c, t), kv_at(c, cp, t), fs.at[c[0], t, d], fr.at[c[0], t, d], to) for t in TWO for d, to in enumerate((*ends, partner))]

    def kv_second(c):
        refs = [kv_at(c, (behind, ahead)[d], d) for d in TWO]
        return [send(refs[d], refs[d], hs.at[c[0], d], hr.at[c[0], d], ends[d]) for d in TWO]

    def kv_relay(c, e):
        refs = [kv_at(c, (behind, ahead, across)[e], t) for t in TWO]
        return [send(refs[t], refs[t], ps.at[c[0], e, t], pr.at[c[0], e, t], partner) for t in TWO]

    def stores(c):
        k, first, size = c
        at, slot, some = span(first, size), lax.rem(k, depth), head_of(size)
        pairs = [(kv_mine(c, t), kv_at(c, cp, t)) for t in TWO] + [(nbuf.at[slot, t, some, :], (k_hbm, v_hbm)[t].at[1, at, :]) for t in TWO]
        pairs += [(nbuf.at[slot, PAIR + t, some, :], q_hbm.at[at, pl.ds(t * nw, nw)]) for t in range(n_qt)]
        return [pltpu.make_async_copy(src, dst, nsem.at[slot, t]) for t, (src, dst) in enumerate(pairs)]

    def f0(c, base):
        k, first, size = c
        at, slot, some = span(first, size), lax.rem(k, depth), head_of(size)
        load = [pltpu.make_async_copy(out_hbm.at[at, :], xbuf.at[some, :], xsem)]
        start(load)
        wait(load)
        sub = 32

        @pl.loop(0, size // sub)
        def _(i):
            rows_of = span(i * sub, sub)
            xf = xbuf[rows_of, :].astype(F32)
            mbuf[rows_of, :] = (xf * mean_scale(xf) * hg_ref[...]).astype(BF)

        cosine, sine = cos_ref[at, :], sin_ref[at, :]
        for t in range(n_n):
            start_w(base + t + PAIR)
            w_slot = lax.rem(base + t, depth)
            pltpu.make_async_copy(wk_hbm.at[layer + 1], narrow(w_slot), wsem.at[w_slot, 0]).wait()
            acc = jnp.dot(mbuf[some, :], narrow(w_slot)[...], preferred_element_type=F32)
            if t == 1:
                nbuf[slot, t, some, :] = acc.astype(BF)
                vbuf[slot, :, some] = acc.T.astype(BF)
                start(kv_first(c))
            else:
                for begin in range(0, nw, dim):
                    this = slice(begin, begin + dim)
                    nbuf[slot, t, some, this] = rotate_heads(acc[:, this], qg_ref[...] if t else kg_ref[...], cosine, sine)
        start(stores(c))

    def f1(c):
        arrived(kv_first(c))
        start(kv_second(c), *[kv_relay(c, e) for e in TWO])

    def f2(c):
        arrived(kv_second(c))
        start(kv_relay(c, PAIR))
        departed(kv_first(c))
        wait(stores(c))

    def f3(c):
        wait(*[kv_relay(c, e) for e in TRIO])
        departed(kv_second(c))

    piece = o_width // n_cp

    def strips(s, dev, size=piece, part=0):
        return wn_hbm.at[lax.rem(me + 1 + s, n_tp), span(dev * piece + part * size, size), :]

    def a_first(s):
        ref = strips(s, cp)
        return [send(ref, ref, a1s.at[s, d], a1r.at[s, d], ends[d]) for d in TWO]

    def a_second(s):
        refs = [strips(s, (behind, ahead)[d], piece // PAIR, d) for d in TWO]
        return [send(refs[d], refs[d], a2s.at[s, d], a2r.at[s, d], ends[d]) for d in TWO]

    def a_relay(s, *kinds):
        refs = {e: strips(s, (cp, behind, ahead, across)[e]) for e in kinds}
        return [send(ref, ref, bs.at[s, e], br_.at[s, e], partner) for e, ref in refs.items()]

    def a_serve(s):
        arrived(a_first(s))
        start(a_second(s), a_relay(s, *TRIO[1:]))

    def a_finish(s):
        arrived(a_second(s))
        start(a_relay(s, len(TRIO)))

    def a_drain(s):
        wait(a_relay(s, *TRIO, len(TRIO)))
        departed(a_first(s), a_second(s))

    for t in TWO:
        start_w(jnp.int32(t))
    greet((*sides, *ends, partner) if follow else sides)
    start(*[o_first(ready + t) for t in TWO])
    if follow:
        for s in TRIO:
            start(a_first(s), a_relay(s, 0))
    served = ready
    if not ready:
        for served in TWO:
            o_serve(served)
        served = PAIR

    def serve(n, place):
        if served + place < units:
            @pl.when(n == 0)
            def _():
                o_serve(served + place)

    def load_rows(n):
        at = span(n * tm, tm)
        copies = [pltpu.make_async_copy(x_hbm.at[at, :], xbuf, xsem)]
        for s in range(n_tp):
            src = og_hbm.at[s - 1] if s else o_hbm
            copies.append(pltpu.make_async_copy(src.at[at, :], obuf.at[:, pl.ds(s * o_width, o_width)], osem.at[s]))
        return copies

    def chunk(n, _):
        base = base_of(n)
        slot_p = lax.rem(n, PAIR)
        p = pbuf.at[slot_p]

        @pl.when(n * tm >= ready * unit)
        def _():
            all_of(o_finish, n)

        start(load_rows(n))
        wait(load_rows(n))

        @pl.loop(0, n_o)
        def _(j):
            start_w(base + j + PAIR)
            slot = wait_wo(base + j)
            p[:, columns(j)] = jnp.dot(obuf[...], wbuf[slot], preferred_element_type=F32)

            @pl.when(j == n_o // PAIR)
            def _():
                serve(n, 0)

        serve(n, 1)

        if follow:
            @pl.when(n > lag)
            def _():
                f1(batch(n - 1 - lag))

        sub = 32

        @pl.loop(0, tm // sub)
        def _(i):
            at = span(i * sub, sub)
            z = p[at, :]
            r = (xbuf[at, :].astype(F32) + z * mean_scale(z) * gain_ref[0:1, :]).astype(BF)
            xbuf[at, :] = r
            rf = r.astype(F32)
            mbuf[at, :] = (rf * mean_scale(rf) * gain_ref[1:2, :]).astype(BF)

        for i in range(fine):
            rown[slot_p, i] = xbuf[span(i * unit + me * br, br), :]

        @pl.loop(0, n_g)
        def _(j):
            index = base + n_o + PAIR * j
            start_w(index + PAIR)
            slot = wait_w(index, width)
            gate = jnp.dot(mbuf[...], part_of(slot, width)[...], preferred_element_type=F32)
            start_w(index + depth)
            slot = wait_w(index + 1, width)
            up = jnp.dot(mbuf[...], part_of(slot, width)[...], preferred_element_type=F32)
            sbuf[:, columns(j)] = (jax.nn.gelu(gate, approximate=True) * up).astype(BF)

            @pl.when((j == 0) & (n >= 1))
            def _():
                all_of(e1, n - 1)
                if follow:
                    a_serve(n - 1)

            @pl.when(j == 1)
            def _():
                serve(n, PAIR)

                @pl.when(n >= lag)
                def _():
                    all_of(e3, n - lag)

            @pl.when(j == depth)
            def _():
                serve(n, depth)

        @pl.when(n >= 1)
        def _():
            all_of(e2, n - 1)

        if follow:
            @pl.when(n > lag)
            def _():
                f2(batch(n - 1 - lag))

        @pl.loop(0, n_d)
        def _(j):
            index = base + n_og + j
            start_w(index + PAIR)
            slot = wait_w(index, hidden)
            p[:, columns(j)] = jnp.dot(sbuf[...], part_of(slot, hidden)[...], preferred_element_type=F32)

            @pl.when(j == 0)
            def _():
                serve(n, 4)

        serve(n, 5)
        e0(n)

        @pl.when(n >= lag)
        def _():
            all_of(e4, n - lag)
            if follow:
                f0(batch(n - lag), base + per)

        return 0

    lax.fori_loop(0, chunks, chunk, 0)
    every = [jnp.int32(k) for k in range(chunks)]
    tail = jnp.int32(total - depth * n_n)
    *_, before, last = every
    all_of(e1, last)
    all_of(e3, before)
    if follow:
        early, middle, *late = *map(batch, every[1:-1]), *ends_of
        f1(early)
    all_of(e2, last)
    all_of(e4, before)
    if follow:
        f2(early)
        f0(middle, tail)
    all_of(e3, last)
    if follow:
        each_strip = lambda step: [step(s) for s in TRIO]
        each_strip(a_finish)
        for i, c in enumerate(late):
            e4(last * fine + i)
            f0(c, tail + (1 + i) * n_n)
            (f2 if i else f1)(middle)
        for step in (f1, f2):
            for c in late:
                step(c)
        each_strip(a_drain)
        for c in (batch(every[0]), early, middle, *late):
            f3(c)
    else:
        all_of(e4, last)


def block_call(layer, n_tp, n_cp, o, w_o, wo_all, x, w_gate, w_up, w_down, gain, gathered=None, following=None):
    rows, width = x.shape
    o_width = o.shape[1]
    hidden = w_down.shape[1]
    tm, nt, unit = TILE, 768, LANES
    chunks, br, units = rows // tm, unit // n_tp, rows // unit
    vmem = pl.BlockSpec(memory_space=VM)
    deep = max(n_tp * o_width, width, hidden)
    shape = lambda *sizes: jax.ShapeDtypeStruct(sizes, BF)
    operands = [o, w_o, wo_all, x, w_gate, w_up, w_down, gain]
    in_specs = [ANY] * 7 + [vmem]
    out_shape = [shape(rows, width), shape(n_tp - 1, rows, o_width)]
    scratch = [
        VM((3, deep, nt), BF), VM((PAIR, tm, width), F32), VM((units, PAIR, br, width // PAIR), F32), VM((units, PAIR, br, width), F32),
        VM((units, br, width), BF), VM((tm, width), BF), VM((tm, hidden), BF), VM((tm, n_tp * o_width), BF), VM((tm, width), BF), VM((PAIR, tm // unit, br, width), BF),
        DMA((3, n_tp)), DMA((n_tp,)), DMA, DMA((units,)),
    ] + [DMA((units, PAIR))] * 14
    aliases = {}
    if gathered is not None:
        aliases[len(operands)] = 1
        operands.append(gathered)
        in_specs.append(ANY)
    if following is not None:
        q_width, kv_width = following[0].shape[-1], following[1].shape[-1]
        n_qt = q_width // kv_width
        operands += following
        in_specs += [ANY] * 3 + [vmem] * 5 + [ANY] * 3
        kept = following[-3:]
        out_shape += [shape(rows, q_width), shape(n_cp * rows, kv_width), shape(kv_width, n_cp * rows)] + [shape(*a.shape) for a in kept]
        aliases.update((len(operands) - i, len(out_shape) - i) for i in range(1, 1 + len(kept)))
        scratch += [VM((3, n_qt + PAIR, tm, kv_width), BF), VM((3, kv_width, tm), BF), DMA((3, n_qt + 4))]
        late = chunks + 1
        for count, sizes in ((1, (late, PAIR, 3)), (1, (late, PAIR)), (1, (late, 3, PAIR)), (PAIR, (n_tp - 1, PAIR)), (1, (n_tp - 1, 4))):
            scratch += [DMA(sizes)] * (PAIR * count)
    weights = width * (n_tp * o_width + 3 * hidden)
    return pl.pallas_call(
        functools.partial(block_kernel, layer, n_tp, n_cp, tm, nt, unit, 0 if gathered is None else units // PAIR, following is not None),
        in_specs=in_specs,
        out_specs=[ANY] * len(out_shape),
        out_shape=out_shape,
        scratch_shapes=scratch,
        input_output_aliases=aliases,
        compiler_params=pltpu.CompilerParams(collective_id=layer, has_side_effects=True, vmem_limit_bytes=BIG_VMEM),
        cost_estimate=pl.CostEstimate(flops=4 * rows * weights, bytes_accessed=8 * weights, transcendentals=0),
        name=f"block_{layer}",
    )(*operands)


def angles_of(positions, dim, theta):
    inv_freq = theta ** (-(jnp.arange(dim // 2, dtype=F32) * 2.0) / dim)
    angles = positions.astype(F32)[..., None] * inv_freq
    return jnp.cos(angles), jnp.sin(angles)


def solution(mesh):
    n_cp, n_tp = mesh.shape['cp'], mesh.shape['tp']
    row_spec = P(('dp', 'cp'), None)
    col_spec = P(None, None, 'tp')
    row_w_spec = P(None, 'tp', None)
    cache_spec = P(None, ('dp', 'cp'), 'tp', None)

    def device_fn(hidden, positions, w_q, w_k, w_v, w_o, w_gate, w_up, w_down, norm_gain, qk_gain):
        rows, width = hidden.shape
        dim = qk_gain.shape[-1]
        n_kv = w_k.shape[-1] // dim
        gains = 1.0 + norm_gain
        head_gains = 1.0 + qk_gain
        angles = [angles_of(positions, dim, theta) for theta in THETAS]
        norms = [(gains[l, :1], head_gains[l, :1], head_gains[l, 1:], *angles[l]) for l in TWO]
        o_0, k_cache, v_cache, wo_0, wo_1 = first_call(n_tp, n_cp, hidden, w_q, w_k, w_v, w_o, *norms[0])
        following = [w_q, w_k, w_v, *norms[1], k_cache, v_cache, wo_1]
        x_1, _, q_1, k_all, vt_all, k_cache, v_cache, wo_1 = block_call(0, n_tp, n_cp, o_0, w_o, wo_0, hidden, w_gate, w_up, w_down, gains[0, 1:], following=following)
        o_1, gathered = global_call(n_tp, q_1, k_all, vt_all, dim)
        x_2, _ = block_call(1, n_tp, n_cp, o_1, w_o, wo_1, x_1, w_gate, w_up, w_down, gains[1, 1:], gathered=gathered)
        return x_2, *[a.reshape(PAIR, rows, n_kv, dim) for a in (k_cache, v_cache)]

    return jax.shard_map(
        device_fn,
        mesh=mesh,
        in_specs=(row_spec, P(('dp', 'cp')), col_spec, col_spec, col_spec, row_w_spec, col_spec, col_spec, row_w_spec, P(), P()),
        out_specs=(row_spec, cache_spec, cache_spec),
        check_vma=False,
    )
```

```python
import functools
import types
import jax
import jax.numpy as jnp
from jax import lax
from jax.experimental import pallas as pl
from jax.experimental.pallas import tpu as pltpu
from jax.sharding import PartitionSpec as P

WINDOW = 1024
THETAS = (10000.0, 1000000.0)
EPS = 1e-6
NEG_BIG = -1e30
BF = jnp.bfloat16
F32 = jnp.float32
MESH = pl.DeviceIdType.MESH
ANY = pl.BlockSpec(memory_space=pl.ANY)
LOG2E = 1.4426950408889634
PAIR = 2
TWO = (0, 1)
TRIO = (0, 1, 2)
TILE = 256
LANES = 128
BIG_VMEM = 67_000_000
DMA = pltpu.SemaphoreType.DMA
VM = pltpu.VMEM
GATHER_SEMS = [DMA((3, PAIR))] * 8 + [DMA((6, 3))] * PAIR


def span(start, size, unit=16):
    return pl.ds(pl.multiple_of(start, unit), size)


def send(src, dst, sent, received, to):
    return pltpu.make_async_remote_copy(src_ref=src, dst_ref=dst, send_sem=sent, recv_sem=received, device_id=to, device_id_type=MESH)


def each(method, *groups):
    for group in groups:
        for item in group:
            getattr(item, method)()


def start(*groups):
    each('start', *groups)


def wait(*groups):
    each('wait', *groups)


def arrived(*groups):
    each('wait_recv', *groups)


def departed(*groups):
    each('wait_send', *groups)


def greet(peers):
    barrier = pltpu.get_barrier_semaphore()
    for to in peers:
        pl.semaphore_signal(barrier, inc=1, device_id=to, device_id_type=MESH)
    pl.semaphore_wait(barrier, len(peers))


def gain_of(ref, layer, row):
    return 1.0 + ref[layer, row:row + 1, :]


def around(axis, n, *distances):
    return [lax.rem(lax.axis_index(axis) + n + d, n) for d in distances]


def tp_peers(n_tp):
    return around('tp', n_tp, 1, -1, PAIR)


def cp_peers(n_cp):
    cp = lax.axis_index('cp')
    return (*around('cp', n_cp, PAIR, -PAIR, PAIR * PAIR), cp + 1 - PAIR * lax.rem(cp, PAIR))


def head_of(size):
    return pl.ds(0, size)


def on(axis, *devices):
    return [{axis: dev} for dev in devices]


def mean_scale(values):
    return lax.rsqrt(jnp.mean(values * values, axis=-1, keepdims=True) + EPS)


def rotate_heads(values, gain, cosine, sine):
    half = cosine.shape[-1]
    normed = values * mean_scale(values) * gain
    lower, upper = normed[:, :half], normed[:, half:]
    return jnp.concatenate([lower * cosine - upper * sine, upper * cosine + lower * sine], axis=-1).astype(BF)


def weight_gather(n_tp, n_cp, strip, cut, shard, whole, y1s, y1r, y2s, y2r, x1s=None, x1r=None, x2s=None, x2r=None, rs=None, rr=None):
    n_x = n_cp // PAIR
    half = whole.shape[1] // PAIR
    shared = (half - n_x * strip) // PAIR
    me, cp = lax.axis_index('tp'), lax.axis_index('cp')
    chip, base = cp // PAIR, lax.rem(cp, PAIR) * half
    right, left, opposite = tp_peers(n_tp)
    sides, sources = on('tp', right, left), (left, right, opposite)
    *ends, _, partner = on('cp', *cp_peers(n_cp))

    def strip_of(distance):
        return base + PAIR * shared + lax.rem(chip + n_x + distance, n_x) * strip

    pieces = ((strip_of(0), strip, strip // PAIR), (base, shared, shared // PAIR), (base + shared, shared, shared // PAIR))
    count = len(pieces)

    def halves(first, size, cut):
        return span(first, cut), span(first + cut, size - cut)

    def y_first(p):
        at = span(*pieces[p][:PAIR])
        return [send(shard.at[at, :], whole.at[me, at, :], y1s.at[p, d], y1r.at[p, d], sides[d]) for d in TWO]

    def y_second(p):
        refs = [whole.at[sources[d], halves(*pieces[p])[d], :] for d in TWO]
        return [send(refs[d], refs[d], y2s.at[p, d], y2r.at[p, d], sides[d]) for d in TWO]

    def x_first(s):
        ref = whole.at[sources[s], span(strip_of(0), strip), :]
        return [send(ref, ref, x1s.at[s, d], x1r.at[s, d], ends[d]) for d in TWO]

    def x_second(s):
        refs = [whole.at[sources[s], halves(strip_of((-1, 1)[d]), strip, cut)[d], :] for d in TWO]
        return [send(refs[d], refs[d], x2s.at[s, d], x2r.at[s, d], ends[d]) for d in TWO]

    def relay(kind, s):
        first, size = pieces[kind][:PAIR] if kind < count else (strip_of(kind + 1 - count), strip)
        ref = whole.at[sources[s], span(first, size), :]
        return [send(ref, ref, rs.at[kind, s], rr.at[kind, s], partner)]

    def y_stage(p, *more):
        arrived(y_first(p))
        start(y_second(p), *more, *[relay(p, s) for s in TWO])

    def y_end(p):
        arrived(y_second(p))
        start(relay(p, PAIR))

    def x_stage(s):
        arrived(x_first(s))
        start(x_second(s), relay(count, s), relay(count + PAIR, s))

    def x_end(s):
        arrived(x_second(s))
        start(relay(count + 1, s))

    def drain(parts):
        for s in TRIO:
            wait(*[relay(kind, s) for kind in range(PAIR * count)])
            departed(x_first(s), x_second(s))
        for p in parts:
            departed(y_first(p), y_second(p))

    peers = (*sides, *ends, partner)
    return types.SimpleNamespace(**{f.__name__: f for f in (y_first, y_second, x_first, x_second, relay, y_stage, y_end, x_stage, x_end, drain)}, peers=peers)


def keep_heads(rows_ref, out_ref):
    dim = out_ref.shape[-1]

    @pl.loop(0, out_ref.shape[1] // LANES)
    def _(i):
        at = span(i * LANES, LANES)
        for t in TWO:
            out_ref[t, at] = jnp.stack([rows_ref[t, at, begin:begin + dim] for begin in range(0, rows_ref.shape[-1], dim)], axis=1)


def first_kernel(
    n_q, n_kv, n_tp, n_cp, strip, cut,
    x_ref, wk_ref, wv_ref, wq_ref, gain_ref, hg_ref, cos_ref, sin_ref, wo_hbm,
    o_hbm, kc_hbm, vc_hbm, wo_all,
    h_ref, q_ref, kv_ref, past_ref, cache_ref,
    ks, kr, csem, osem, *sems,
):
    step = pl.program_id(0)
    rows = x_ref.shape[0]
    dim = hg_ref.shape[-1]
    g = weight_gather(n_tp, n_cp, strip, cut, wo_hbm.at[0], wo_all, *sems)
    follow, prior = on('cp', *around('cp', n_cp, 1, -1))

    def send_kv(t):
        return [send(kv_ref.at[t], past_ref.at[t], ks.at[t], kr.at[t], follow)]

    def keep_kv(t):
        return [pltpu.make_async_copy(cache_ref.at[t], (kc_hbm, vc_hbm)[t].at[0], csem.at[t])]

    group = n_q // n_kv

    keep_o = [pltpu.make_async_copy(q_ref, o_hbm, osem)]

    q_step = PAIR * n_kv

    @pl.when(step == 0)
    def _():
        greet((*g.peers[:-1], follow, prior))
        start(*map(g.y_first, TWO))
        rb = 32

        @pl.loop(0, rows // rb)
        def _(i):
            at = span(i * rb, rb)
            xf = x_ref[at, :].astype(F32)
            h_ref[at, :] = (xf * mean_scale(xf) * gain_of(gain_ref, 0, 0)).astype(BF)

    @pl.when(step == n_kv)
    def _():
        start(send_kv(0))

    @pl.when(step == q_step)
    def _():
        g.y_stage(0, g.y_first(PAIR), *map(g.x_first, TWO))
        start(send_kv(1))

    @pl.when(step == q_step + 3)
    def _():
        g.x_stage(0)

    def project(w_ref, store, finish):
        @pl.loop(0, rows // TILE)
        def _(i):
            at = span(i * TILE, TILE)
            store(at, finish(jnp.dot(h_ref[at, :], w_ref[0], preferred_element_type=F32), at))

    def into_kv(t, head):
        def store(at, value):
            kv_ref[t, at, span(head * dim, dim, LANES)] = value
        return store

    def into_q(at, value):
        q_ref[at, span((step - q_step) * dim, dim, LANES)] = value

    def rotate(row):
        return lambda a, at: rotate_heads(a, gain_of(hg_ref, 0, row), cos_ref[at, :], sin_ref[at, :])

    @pl.when(step < n_kv)
    def _():
        project(wk_ref, into_kv(0, step), rotate(1))

    @pl.when((step >= n_kv) & (step < q_step))
    def _():
        project(wv_ref, into_kv(1, step - n_kv), lambda a, at: a.astype(BF))

    @pl.when(step >= q_step)
    def _():
        project(wq_ref, into_q, rotate(0))

    @pl.when(step == q_step + n_q - 1)
    def _():
        keep_heads(kv_ref, cache_ref)
        start(*map(keep_kv, TWO))
        g.y_stage(1)
        g.y_end(0)
        start(g.x_first(PAIR))
        g.x_stage(1)
        g.y_stage(PAIR)
        arrived(*map(send_kv, TWO))

        @pl.loop(0, n_kv)
        def _(h):
            head = span(h * dim, dim, LANES)

            @pl.loop(0, group)
            def _(i):
                local_head(q_ref, h * group + i, *[ref.at[t, :, head] for t in TWO for ref in (past_ref, kv_ref)])

            @pl.when(h == 0)
            def _():
                g.x_end(0)
                g.x_stage(PAIR)

        start(keep_o)
        g.x_end(1)
        g.y_end(1)
        g.y_end(PAIR)
        g.x_end(PAIR)
        departed(*map(send_kv, TWO))
        wait(*map(keep_kv, TWO), keep_o)
        g.drain(TRIO)


def first_call(n_tp, n_cp, x, w_q, w_k, w_v, w_o, gain, head_gain, cosine, sine):
    rows, width = x.shape
    dim = head_gain.shape[-1]
    n_q, n_kv = w_q.shape[-1] // dim, w_k.shape[-1] // dim
    at_k = lambda t: jnp.minimum(t, n_kv - 1)
    at_v = lambda t: jnp.clip(t - n_kv, 0, n_kv - 1)
    at_q = lambda t: jnp.maximum(t - PAIR * n_kv, 0)
    whole = lambda a: pl.BlockSpec(a.shape, lambda t: TWO[:1] * a.ndim, pipeline_mode=pl.Buffered(1))
    w_spec = lambda at: pl.BlockSpec((1, width, dim), lambda t: (0, 0, at(t)))
    shape = lambda *sizes: jax.ShapeDtypeStruct(sizes, BF)
    q_width, kv_width = n_q * dim, n_kv * dim
    work = PAIR * width * (q_width + PAIR * kv_width)
    gathered, cache = shape(n_tp, *w_o.shape[1:]), shape(PAIR, rows, n_kv, dim)
    flat = (PAIR, rows, kv_width)
    return pl.pallas_call(
        functools.partial(first_kernel, n_q, n_kv, n_tp, n_cp, 64, 16),
        grid=(n_q + PAIR * n_kv,),
        in_specs=[whole(x), *map(w_spec, (at_k, at_v, at_q)), *map(whole, (gain, head_gain, cosine, sine)), ANY],
        out_specs=[ANY] * 4,
        out_shape=[shape(rows, q_width), cache, cache, gathered],
        scratch_shapes=[VM((rows, width), BF), VM((rows, q_width), BF), VM(flat, BF), VM(flat, BF), VM(cache.shape, BF)]
        + [DMA((PAIR,))] * 3 + [DMA] + GATHER_SEMS,
        compiler_params=pltpu.CompilerParams(dimension_semantics=("arbitrary",), collective_id=2, has_side_effects=True, vmem_limit_bytes=BIG_VMEM),
        cost_estimate=pl.CostEstimate(flops=rows * work, bytes_accessed=work, transcendentals=0),
        name="first",
    )(x, w_k, w_v, w_q, gain, head_gain, cosine, sine, w_o)


def scores_of(q, k):
    return lax.dot_general(q, k, (((1,), (1,)), ((), ())), preferred_element_type=F32)


def local_head(q_ref, head, kp_ref, ko_ref, vp_ref, vo_ref):
    rows, dim = ko_ref.shape
    tile = TILE
    scale = dim ** -0.5 * LOG2E
    opening = lax.axis_index('cp') == 0
    row = lax.broadcasted_iota(jnp.int32, (tile, tile), 0)
    col = lax.broadcasted_iota(jnp.int32, (tile, tile), 1)
    for begin in range(0, rows, tile):
        end = begin + tile
        at = (slice(begin, end), span(head * dim, dim, LANES))
        q = q_ref[at]
        past = scores_of(q, kp_ref[begin:, :])
        here = scores_of(q, ko_ref[:end, :])
        past = jnp.concatenate([jnp.where(col > row, past[:, :tile], NEG_BIG), past[:, tile:]][:1 + (end < rows)], axis=1)
        past = jnp.where(opening, NEG_BIG, past)
        here = jnp.concatenate([here[:, :begin], jnp.where(col <= row, here[:, begin:], NEG_BIG)][begin == 0:], axis=1)
        top = jnp.maximum(*[jnp.max(a, axis=1, keepdims=True) for a in (past, here)])
        probs = [jnp.exp2((a - top) * scale) for a in (past, here)]
        total = sum(jnp.sum(p, axis=1, keepdims=True) for p in probs)
        acc = sum(jnp.dot(p.astype(BF), v, preferred_element_type=F32) for p, v in zip(probs, (vp_ref[begin:, :], vo_ref[:end, :])))
        q_ref[at] = (acc / total).astype(BF)


def fold_rows(values, op):
    return op(values.reshape(-1, 8, values.shape[-1]), axis=0)


def row_gather(n_tp, unit, gathered, own, s1, r1, s2, r2):
    sides = on('tp', *tp_peers(n_tp)[:PAIR])
    half = gathered.shape[-1] // PAIR
    seen = TRIO[::-PAIR]

    def first(u):
        at = span(u * unit, unit)
        return [send(own.at[at, :], gathered.at[seen[d], at, :], s1.at[u, d], r1.at[u, d], sides[d]) for d in TWO]

    def second(u):
        at = span(u * unit, unit)
        cols = [slice(d * half, (d + 1) * half) for d in TWO]
        return [send(gathered.at[seen[d], at, cols[d]], gathered.at[1, at, cols[d]], s2.at[u, d], r2.at[u, d], sides[d]) for d in TWO]

    return sides, first, second


def global_kernel(
    groups, n_tp, n_cp, unit, strip, cut, q_ref, k_hbm, vt_hbm, wo_hbm, _, o_hbm, og_hbm, wn_hbm,
    k_ref, vt_ref, o_ref, m_ref, l_ref, ka_ref, kb_ref, xa_ref, xb_ref, acc_ref, sa_ref, sb_ref, pa_ref, pb_ref,
    ksem, vsem, osem, s1, r1, s2, r2, *sems,
):
    rows, width = q_ref.shape
    dim = acc_ref.shape[0]
    n_kv = k_hbm.shape[1] // dim
    block, wide = sa_ref.shape
    tile = wide // groups
    scale = dim ** -0.5 * LOG2E
    cp = lax.axis_index('cp')
    base = cp * (rows // block)
    last = base - 1
    _, first, second = row_gather(n_tp, unit, og_hbm, o_ref, s1, r1, s2, r2)
    w = weight_gather(n_tp, n_cp, strip, cut, wo_hbm.at[1], wn_hbm, *sems)
    ready = tile // unit

    def load(b):
        at = span(b * rows, rows, LANES)
        return [pltpu.make_async_copy(k_hbm.at[at, :], k_ref.at[at, :], ksem.at[b]), pltpu.make_async_copy(vt_hbm.at[:, at], vt_ref.at[:, at], vsem.at[b])]

    def store(i):
        at = span(i * tile, tile)
        return [pltpu.make_async_copy(o_ref.at[at, :], o_hbm.at[at, :], osem.at[i])]

    start(load(cp))

    @pl.loop(0, cp)
    def _(b):
        start(load(b))

    greet(w.peers)
    start(w.y_first(1), w.y_first(PAIR), *map(w.x_first, TRIO), *[w.relay(0, s) for s in TRIO])
    wait(load(cp))

    key = lax.broadcasted_iota(jnp.int32, (block, wide), 0)
    token = lax.rem(lax.broadcasted_iota(jnp.int32, (block, wide), 1), tile)

    @pl.loop(0, n_kv * (rows // tile))
    def _(turn):
        i, h = turn // n_kv, lax.rem(turn, n_kv)
        head = span(h * dim, dim, LANES)

        q = jnp.concatenate([q_ref[span(i * tile, tile), span((h * groups + g) * dim, dim, LANES)] for g in range(groups)], axis=0)

        def score(b, s_ref, x_ref, masked=False):
            s = scores_of(k_ref[span(b * block, block), head], q)
            if masked:
                s = jnp.where(key <= token, s, NEG_BIG)
            s_ref[...] = s
            x_ref[...] = fold_rows(s, jnp.max)

        def soften(s_ref, x_ref, p_ref, keep_ref, opening=False):
            top = jnp.max(x_ref[...], axis=0, keepdims=True)
            if not opening:
                old = m_ref[...]
                top = jnp.maximum(old, top)
                keep_ref[...] = jnp.exp2((old - top) * scale)
            m_ref[...] = top
            prob = jnp.exp2((s_ref[...] - top) * scale)
            part = fold_rows(prob, jnp.sum)
            l_ref[...] = part if opening else l_ref[...] * keep_ref[...] + part
            p_ref[...] = prob.astype(BF)

        def weigh(b, p_ref, keep_ref, opening=False):
            part = jnp.dot(vt_ref[head, span(b * block, block, LANES)], p_ref[...], preferred_element_type=F32)
            acc_ref[...] = part if opening else acc_ref[...] * keep_ref[...] + part

        score(base + i, sa_ref, xa_ref, True)
        soften(sa_ref, xa_ref, pa_ref, ka_ref, True)
        weigh(base + i, pa_ref, ka_ref, True)

        @pl.loop(0, i)
        def _(b):
            score(base + b, sa_ref, xa_ref)
            soften(sa_ref, xa_ref, pa_ref, ka_ref)
            weigh(base + b, pa_ref, ka_ref)

        def loaded(b):
            @pl.when((turn == 0) & (b < cp))
            def _():
                wait(load(b))

        @pl.when(cp > 0)
        def _():
            loaded(0)
            score(jnp.int32(0), sa_ref, xa_ref)
            pb_ref[...] = jnp.zeros_like(pb_ref)
            kb_ref[...] = jnp.ones_like(kb_ref)

            @pl.loop(0, base // PAIR)
            def _(half):
                b = PAIR * half
                loaded(half + 1)
                score(b + 1, sb_ref, xb_ref)
                soften(sa_ref, xa_ref, pa_ref, ka_ref)
                weigh(jnp.maximum(b - 1, 0), pb_ref, kb_ref)
                score(jnp.minimum(b + PAIR, last), sa_ref, xa_ref)
                soften(sb_ref, xb_ref, pb_ref, kb_ref)
                weigh(b, pa_ref, ka_ref)

            weigh(last, pb_ref, kb_ref)

        out = (acc_ref[...] / jnp.sum(l_ref[...], axis=0, keepdims=True)).T.astype(BF)
        for g in range(groups):
            o_ref[span(i * tile, tile), span((h * groups + g) * dim, dim, LANES)] = out[g * tile:(g + 1) * tile]

        @pl.when(turn == 0)
        def _():
            w.y_stage(1)
            w.x_stage(0)

        @pl.when(turn == n_kv - 1)
        def _():
            start(store(0), *map(first, range(ready)))
            w.y_stage(PAIR)
            w.x_stage(1)

        @pl.when(turn == n_kv)
        def _():
            w.x_stage(PAIR)
            w.y_end(1)
            for u in range(ready - 1):
                arrived(first(u))
                start(second(u))

    start(store(1))
    arrived(first(ready - 1))
    start(second(ready - 1))
    w.x_end(0)
    w.x_end(1)
    w.y_end(PAIR)
    w.x_end(PAIR)
    for u in range(ready):
        departed(first(u))
        wait(second(u))
    wait(*map(store, TWO))
    w.drain(TRIO[1:])


def global_call(n_tp, n_cp, strip, cut, q, k_all, vt_all, w_o, wo_next, dim):
    rows, width = q.shape
    every, kv_width = k_all.shape
    groups = width // kv_width
    tile = rows // PAIR
    wide = groups * tile
    unit = LANES
    vmem = pl.BlockSpec(memory_space=VM)
    row, slab = VM((1, wide), F32), VM((8, wide), F32)
    return pl.pallas_call(
        functools.partial(global_kernel, groups, n_tp, n_cp, unit, strip, cut),
        in_specs=[vmem] + [ANY] * 4,
        out_specs=[ANY] * 3,
        out_shape=[jax.ShapeDtypeStruct(size, BF) for size in (q.shape, (n_tp - 1, *q.shape), wo_next.shape)],
        input_output_aliases={4: PAIR},
        scratch_shapes=[VM(k_all.shape, BF), VM(vt_all.shape, BF), VM(q.shape, BF), row, slab, row, row, slab, slab, VM((dim, wide), F32)]
        + [VM((tile, wide), t) for t in (F32, F32, BF, BF)] + [DMA((every // rows,))] * PAIR + [DMA((PAIR,))] + [DMA((tile // unit, PAIR))] * 4 + GATHER_SEMS,
        compiler_params=pltpu.CompilerParams(collective_id=3, has_side_effects=True, vmem_limit_bytes=BIG_VMEM),
        cost_estimate=pl.CostEstimate(flops=PAIR * rows * every * width, bytes_accessed=PAIR * every * width, transcendentals=0),
        name="attend_global",
    )(q, k_all, vt_all, w_o, wo_next)


def block_kernel(layer, n_tp, n_cp, tm, nt, unit, strip, cut, ready, follow, *refs):
    queue = iter(refs)

    def take(names):
        return [ref for _, ref in zip(range(names), queue)]

    o_hbm, wo_own, wo_hbm, x_hbm, wg_hbm, wu_hbm, wd_hbm, gain_ref = take(8)
    if ready:
        take(1)
    if follow:
        wq_hbm, wk_hbm, wv_hbm, hg_ref, cos_ref, sin_ref, *_ = take(8)
    out_hbm, og_hbm = take(PAIR)
    if follow:
        q_hbm, ka_hbm, va_hbm, k_hbm, v_hbm, wn_hbm = take(6)
    wbuf, pbuf, r1, r2, xb, mbuf, sbuf, gbuf, obuf, xbuf, rown, wsem, osem, xsem, stsem = take(15)
    o1s, o1r, o2s, o2r, s1s, s1r, sbs, sbr, sas, sar, g1s, g1r, g2s, g2r = take(14)
    if follow:
        nbuf, vbuf, cbuf, nsem, fs, fr, hs, hr, ps, pr, *sems = take(14)
        w = weight_gather(n_tp, n_cp, strip, cut, wo_own.at[layer + 1], wn_hbm, *sems)

    rows, width = x_hbm.shape
    o_width = o_hbm.shape[1]
    hidden = wd_hbm.shape[1]
    chunks = rows // tm
    fine = tm // unit
    br = unit // n_tp
    hw = width // PAIR
    units = rows // unit
    n_o, n_g, n_d = width // nt, hidden // nt, width // nt
    n_og = n_o + PAIR * n_g
    per = n_og + n_d
    depth, lag = 3, PAIR
    n_n = 0
    if follow:
        dim = hg_ref.shape[-1]
        nw = wk_hbm.shape[-1]
        n_qt = wq_hbm.shape[-1] // nw
        n_n = n_qt + PAIR
    total = chunks * per + (chunks + 1) * n_n

    me, cp = lax.axis_index('tp'), lax.axis_index('cp')
    right, left, opposite = tp_peers(n_tp)
    near = (right, left)
    far = (left, right)
    ahead, behind, across, mate = cp_peers(n_cp)
    *ends, partner = on('cp', ahead, behind, mate)
    sides, o_first, o_second = row_gather(n_tp, unit, og_hbm, o_hbm, o1s, o1r, o2s, o2r)

    def base_of(n):
        return n * per + jnp.maximum(n - lag, 0) * n_n

    def step_of(index):
        if not follow:
            return lax.rem(index, per)
        head, body = lag * per, (chunks - lag) * (per + n_n)
        late = index - head
        tail = per + lax.rem(jnp.maximum(late - body, 0), n_n)
        return jnp.where(late < 0, lax.rem(index, per), jnp.where(late < body, lax.rem(jnp.maximum(late, 0), per + n_n), tail))

    def columns(tile):
        return span(tile * nt, nt, LANES)

    def part_of(slot, length, first=0):
        return wbuf.at[slot, pl.ds(first, length), :]

    def narrow(slot):
        return wbuf.at[slot, head_of(width), head_of(nw)]

    def start_w(index):
        step, slot = step_of(index), lax.rem(index, depth)

        def load(wanted, src, dst, s=0):
            @pl.when((index < total) & wanted)
            def _():
                pltpu.make_async_copy(src, dst, wsem.at[slot, s]).start()

        for s in range(n_tp):
            src = wo_hbm.at[lax.rem(me + s, n_tp)] if s else wo_own.at[layer]
            load(step < n_o, src.at[:, columns(jnp.minimum(step, n_o - 1))], part_of(slot, o_width, s * o_width), s)
        middle = jnp.clip(step - n_o, 0, n_og - n_o - 1)
        for t, src in enumerate((wg_hbm, wu_hbm)):
            load((step >= n_o) & (step < n_og) & (lax.rem(middle, PAIR) == t), src.at[layer, :, columns(middle // PAIR)], part_of(slot, width))
        load((step >= n_og) & (step < per), wd_hbm.at[layer, :, columns(jnp.clip(step - n_og, 0, n_d - 1))], part_of(slot, hidden))
        if follow:
            for t, src in enumerate((wk_hbm, wv_hbm)):
                load(step == per + t, src.at[layer + 1], narrow(slot))
            late = step - per - PAIR
            load(late >= 0, wq_hbm.at[layer + 1, :, span(jnp.clip(late, 0, n_qt - 1) * nw, nw, LANES)], narrow(slot))

    def wait_w(index, length):
        slot = lax.rem(index, depth)
        pltpu.make_async_copy(wd_hbm.at[layer, head_of(length), columns(0)], part_of(slot, length), wsem.at[slot, 0]).wait()
        return slot

    def wait_wo(index):
        slot = lax.rem(index, depth)
        for s in range(n_tp):
            pltpu.make_async_copy(wo_own.at[layer, :, columns(0)], part_of(slot, o_width, s * o_width), wsem.at[slot, s]).wait()
        return slot

    def o_serve(u):
        arrived(o_first(u))
        start(o_second(u))

        @pl.when(u + PAIR < units)
        def _():
            start(o_first(u + PAIR))

    def o_finish(u):
        departed(o_first(u))
        wait(o_second(u))

    cols = [pl.ds(d * hw, hw) for d in TWO]
    other = cols[::-1]

    def partial(k):
        return pbuf.at[lax.rem(k // fine, PAIR)]

    def part(k, dev):
        return span(lax.rem(k, fine) * unit + dev * br, br)

    def reduce(kind, k, d, dev, side, dst):
        s_sem, r_sem = kind
        return [send(partial(k).at[part(k, dev), side], dst, s_sem.at[k, d], r_sem.at[k, d], sides[d])]

    def s_far(k, d):
        return reduce((s1s, s1r), k, d, opposite, cols[d], r1.at[k, d])

    def s_plain(k, d):
        return reduce((sbs, sbr), k, d, near[d], other[d], r2.at[k, d, :, other[d]])

    def s_sum(k, d):
        return reduce((sas, sar), k, d, near[d], cols[d], r2.at[k, d, :, cols[d]])

    def x_rows(k, dev):
        return span(k * unit + dev * br, br)

    def x_first(k):
        return [send(xb.at[k], out_hbm.at[x_rows(k, me), :], g1s.at[k, d], g1r.at[k, d], sides[d]) for d in TWO]

    def x_second(k):
        refs = [out_hbm.at[x_rows(k, far[d]), cols[d]] for d in TWO]
        return [send(refs[d], refs[d], g2s.at[k, d], g2r.at[k, d], sides[d]) for d in TWO]

    def x_own(k):
        return [pltpu.make_async_copy(xb.at[k], out_hbm.at[x_rows(k, me), :], stsem.at[k])]

    def e0(n):
        for kind in (s_far, s_plain):
            for i in range(fine):
                start(*[kind(n * fine + i, d) for d in TWO])

    def e1(k):
        p = partial(k)
        for d in TWO:
            at = (part(k, near[d]), cols[d])
            arrived(s_far(k, d))
            p[at] = p[at] + r1[k, d]
            start(s_sum(k, d))

    def e2(k):
        p = partial(k)
        for d in TWO:
            arrived(s_plain(k, d), s_sum(k, d))
        sub = 16
        for begin in range(0, br, sub):
            at = pl.ds(begin, sub)
            z = sum([r2[k, d, at, :] for d in TWO], p[span(lax.rem(k, fine) * unit + me * br + begin, sub), :])
            r = rown[lax.rem(k // fine, PAIR), lax.rem(k, fine), at, :].astype(F32)
            xb[k, at, :] = (r + z * mean_scale(z) * gain_of(gain_ref, layer, 3)).astype(BF)
        start(x_first(k), x_own(k))
        for d in TWO:
            departed(s_far(k, d), s_plain(k, d), s_sum(k, d))

    def e3(k):
        arrived(x_first(k))
        start(x_second(k))

    def e4(k):
        wait(x_second(k), x_own(k))
        departed(x_first(k))

    def all_of(step, n):
        for i in range(fine):
            step(n * fine + i)

    def batch(n):
        return n, n * tm, tm

    ends_of = [(jnp.int32(chunks - 1 + i), jnp.int32(rows - tm + i * unit), unit) for i in TWO]

    def kv_at(c, dev, t):
        at = span(dev * rows + c[1], c[PAIR], LANES)
        return va_hbm.at[:, at] if t else ka_hbm.at[at, :]

    def kv_mine(c, t):
        slot, some = lax.rem(c[0], depth), head_of(c[PAIR])
        return vbuf.at[slot, :, some] if t else nbuf.at[slot, 0, some, :]

    def kv_first(c):
        return [send(kv_mine(c, t), kv_at(c, cp, t), fs.at[c[0], t, d], fr.at[c[0], t, d], to) for t in TWO for d, to in enumerate((*ends, partner))]

    def kv_second(c):
        refs = [kv_at(c, (behind, ahead)[d], d) for d in TWO]
        return [send(refs[d], refs[d], hs.at[c[0], d], hr.at[c[0], d], ends[d]) for d in TWO]

    def kv_relay(c, e):
        refs = [kv_at(c, (behind, ahead, across)[e], t) for t in TWO]
        return [send(refs[t], refs[t], ps.at[c[0], e, t], pr.at[c[0], e, t], partner) for t in TWO]

    def stores(c):
        k, first, size = c
        at, slot, some = span(first, size), lax.rem(k, depth), head_of(size)
        pairs = [(kv_mine(c, t), kv_at(c, cp, t)) for t in TWO] + [(cbuf.at[slot, t, some], (k_hbm, v_hbm)[t].at[1, at]) for t in TWO]
        pairs += [(nbuf.at[slot, PAIR + t, some, :], q_hbm.at[at, pl.ds(t * nw, nw)]) for t in range(n_qt)]
        return [pltpu.make_async_copy(src, dst, nsem.at[slot, t]) for t, (src, dst) in enumerate(pairs)]

    def f0(c, base):
        k, first, size = c
        at, slot, some = span(first, size), lax.rem(k, depth), head_of(size)
        load = [pltpu.make_async_copy(out_hbm.at[at, :], xbuf.at[some, :], xsem)]
        start(load)
        wait(load)
        sub = 32

        @pl.loop(0, size // sub)
        def _(i):
            rows_of = span(i * sub, sub)
            xf = xbuf[rows_of, :].astype(F32)
            mbuf[rows_of, :] = (xf * mean_scale(xf) * gain_of(gain_ref, layer + 1, 0)).astype(BF)

        cosine, sine = cos_ref[at, :], sin_ref[at, :]

        def project(t, finish):
            start_w(base + t + PAIR)
            w_slot = lax.rem(base + t, depth)
            pltpu.make_async_copy(wk_hbm.at[layer + 1], narrow(w_slot), wsem.at[w_slot, 0]).wait()

            @pl.loop(0, nw // dim)
            def _(h):
                this = span(h * dim, dim, LANES)
                finish(this, jnp.dot(mbuf[some, :], wbuf[w_slot, head_of(width), this], preferred_element_type=F32))

        def rotate(t, row):
            def finish(this, acc):
                nbuf[slot, t, some, this] = rotate_heads(acc, gain_of(hg_ref, layer + 1, row), cosine, sine)
            return finish

        def plain(this, acc):
            nbuf[slot, 1, some, this] = acc.astype(BF)
            vbuf[slot, this, some] = acc.T.astype(BF)

        project(0, rotate(0, 1))
        project(1, plain)
        start(kv_first(c))

        @pl.loop(PAIR, n_n)
        def _(t):
            project(t, rotate(t, 0))

        keep_heads(nbuf.at[slot, :, some], cbuf.at[slot, :, some])
        start(stores(c))

    def f1(c):
        arrived(kv_first(c))
        start(kv_second(c), *[kv_relay(c, e) for e in TWO])

    def f2(c):
        arrived(kv_second(c))
        start(kv_relay(c, PAIR))
        departed(kv_first(c))
        wait(stores(c))

    def f3(c):
        wait(*[kv_relay(c, e) for e in TRIO])
        departed(kv_second(c))

    for t in TWO:
        start_w(jnp.int32(t))
    greet((*sides, *ends, partner) if follow else sides)
    start(*[o_first(ready + t) for t in TWO])
    served = ready
    if not ready:
        for served in TWO:
            o_serve(served)
        served = PAIR

    def serve(n, place):
        if served + place < units:
            @pl.when(n == 0)
            def _():
                o_serve(served + place)

    def load_rows(n):
        at = span(n * tm, tm)
        copies = [pltpu.make_async_copy(x_hbm.at[at, :], xbuf, xsem)]
        for s in range(n_tp):
            src = og_hbm.at[s - 1] if s else o_hbm
            copies.append(pltpu.make_async_copy(src.at[at, :], obuf.at[:, pl.ds(s * o_width, o_width)], osem.at[s]))
        return copies

    def between(n, j):
        @pl.when((j == 0) & (n >= 1))
        def _():
            all_of(e1, n - 1)

        @pl.when(j == 1)
        def _():
            serve(n, PAIR)

            @pl.when(n >= lag)
            def _():
                all_of(e3, n - lag)

        @pl.when(j == depth)
        def _():
            serve(n, depth)

    def chunk(n, _):
        base = base_of(n)
        slot_p = lax.rem(n, PAIR)
        p = pbuf.at[slot_p]

        @pl.when(n * tm >= ready * unit)
        def _():
            all_of(o_finish, n)

        start(load_rows(n))
        wait(load_rows(n))

        @pl.loop(0, n_o)
        def _(j):
            start_w(base + j + PAIR)
            slot = wait_wo(base + j)
            p[:, columns(j)] = jnp.dot(obuf[...], wbuf[slot], preferred_element_type=F32)

            @pl.when(j == n_o // PAIR)
            def _():
                serve(n, 0)

        serve(n, 1)

        if follow:
            @pl.when(n > lag)
            def _():
                f1(batch(n - 1 - lag))

        sub = 32

        @pl.loop(0, tm // sub)
        def _(i):
            at = span(i * sub, sub)
            z = p[at, :]
            r = (xbuf[at, :].astype(F32) + z * mean_scale(z) * gain_of(gain_ref, layer, 1)).astype(BF)
            xbuf[at, :] = r
            rf = r.astype(F32)
            mbuf[at, :] = (rf * mean_scale(rf) * gain_of(gain_ref, layer, PAIR)).astype(BF)

        for i in range(fine):
            rown[slot_p, i] = xbuf[span(i * unit + me * br, br), :]

        @pl.loop(0, PAIR * n_g)
        def _(t):
            index, j, odd = base + n_o + t, t // PAIR, lax.rem(t, PAIR)
            start_w(index + PAIR)
            slot = wait_w(index, width)
            gbuf[odd] = jnp.dot(mbuf[...], part_of(slot, width)[...], preferred_element_type=F32)

            @pl.when(odd == 1)
            def _():
                sbuf[:, columns(j)] = (jax.nn.gelu(gbuf[0], approximate=True) * gbuf[1]).astype(BF)
                between(n, j)

        @pl.when(n >= 1)
        def _():
            all_of(e2, n - 1)

        if follow:
            @pl.when(n > lag)
            def _():
                f2(batch(n - 1 - lag))

        @pl.loop(0, n_d)
        def _(j):
            index = base + n_og + j
            start_w(index + PAIR)
            slot = wait_w(index, hidden)
            p[:, columns(j)] = jnp.dot(sbuf[...], part_of(slot, hidden)[...], preferred_element_type=F32)

            @pl.when(j == 0)
            def _():
                serve(n, 4)

        serve(n, 5)
        e0(n)

        @pl.when(n >= lag)
        def _():
            all_of(e4, n - lag)
            if follow:
                f0(batch(n - lag), base + per)

        return 0

    lax.fori_loop(0, chunks, chunk, 0)
    every = [jnp.int32(k) for k in range(chunks)]
    tail = jnp.int32(total - depth * n_n)
    *_, before, last = every
    all_of(e1, last)
    all_of(e3, before)
    if follow:
        early, middle, *late = *map(batch, every[1:-1]), *ends_of
        f1(early)
    all_of(e2, last)
    all_of(e4, before)
    if follow:
        f2(early)
        f0(middle, tail)
    all_of(e3, last)
    if follow:
        start(w.y_first(0))

        @pl.loop(0, fine)
        def _(i):
            e4(last * fine + i)
            f0((chunks - 1 + i, rows - tm + i * unit, unit), tail + (1 + i) * n_n)
            for t, step in enumerate((f1, f2)):
                @pl.when(i == t)
                def _():
                    step(middle)

        arrived(w.y_first(0))
        start(w.y_second(0))
        for step in (f1, f2):
            for c in late:
                step(c)
        arrived(w.y_second(0))
        departed(w.y_first(0), w.y_second(0))
        for c in (batch(every[0]), early, middle, *late):
            f3(c)
    else:
        all_of(e4, last)


def block_call(layer, n_tp, n_cp, strip, cut, o, w_o, wo_all, x, w_gate, w_up, w_down, gain, gathered=None, following=None):
    rows, width = x.shape
    o_width = o.shape[1]
    hidden = w_down.shape[1]
    tm, nt, unit = TILE, 768, LANES
    chunks, br, units = rows // tm, unit // n_tp, rows // unit
    vmem = pl.BlockSpec(memory_space=VM)
    deep = max(n_tp * o_width, width, hidden)
    shape = lambda *sizes: jax.ShapeDtypeStruct(sizes, BF)
    operands = [o, w_o, wo_all, x, w_gate, w_up, w_down, gain]
    in_specs = [ANY] * 7 + [vmem]
    out_shape = [shape(rows, width), shape(n_tp - 1, rows, o_width)]
    scratch = [
        VM((3, deep, nt), BF), VM((PAIR, tm, width), F32), VM((units, PAIR, br, width // PAIR), F32), VM((units, PAIR, br, width), F32),
        VM((units, br, width), BF), VM((tm, width), BF), VM((tm, hidden), BF), VM((PAIR, tm, nt), F32), VM((tm, n_tp * o_width), BF), VM((tm, width), BF), VM((PAIR, tm // unit, br, width), BF),
        DMA((3, n_tp)), DMA((n_tp,)), DMA, DMA((units,)),
    ] + [DMA((units, PAIR))] * 14
    aliases = {}
    if gathered is not None:
        aliases[len(operands)] = 1
        operands.append(gathered)
        in_specs.append(ANY)
    if following is not None:
        q_width, kv_width = following[0].shape[-1], following[1].shape[-1]
        n_qt = q_width // kv_width
        operands += following
        in_specs += [ANY] * 3 + [vmem] * 3 + [ANY] * PAIR
        kept = following[-PAIR:]
        out_shape += [shape(rows, q_width), shape(n_cp * rows, kv_width), shape(kv_width, n_cp * rows)] + [shape(*a.shape) for a in kept]
        aliases.update((len(operands) - i, len(out_shape) - i) for i in range(1, 1 + len(kept)))
        out_shape.append(shape(*wo_all.shape))
        scratch += [VM((3, n_qt + PAIR, tm, kv_width), BF), VM((3, kv_width, tm), BF), VM((3, PAIR, tm, *kept[0].shape[PAIR:]), BF), DMA((3, n_qt + 4))]
        late = chunks + 1
        for count, sizes in ((1, (late, PAIR, 3)), (1, (late, PAIR)), (1, (late, 3, PAIR)), (PAIR, (1, PAIR))):
            scratch += [DMA(sizes)] * (PAIR * count)
    weights = width * (n_tp * o_width + 3 * hidden)
    return pl.pallas_call(
        functools.partial(block_kernel, layer, n_tp, n_cp, tm, nt, unit, strip, cut, 0 if gathered is None else units // PAIR, following is not None),
        in_specs=in_specs,
        out_specs=[ANY] * len(out_shape),
        out_shape=out_shape,
        scratch_shapes=scratch,
        input_output_aliases=aliases,
        compiler_params=pltpu.CompilerParams(collective_id=layer, has_side_effects=True, vmem_limit_bytes=BIG_VMEM),
        cost_estimate=pl.CostEstimate(flops=4 * rows * weights, bytes_accessed=8 * weights, transcendentals=0),
        name=f"block_{layer}",
    )(*operands)


def angles_of(positions, dim, theta):
    inv_freq = theta ** (-(jnp.arange(dim // 2, dtype=F32) * 2.0) / dim)
    angles = positions.astype(F32)[..., None] * inv_freq
    return jnp.cos(angles), jnp.sin(angles)


def solution(mesh):
    n_cp, n_tp = mesh.shape['cp'], mesh.shape['tp']
    row_spec = P(('dp', 'cp'), None)
    col_spec = P(None, None, 'tp')
    row_w_spec = P(None, 'tp', None)
    cache_spec = P(None, ('dp', 'cp'), 'tp', None)

    def device_fn(hidden, positions, w_q, w_k, w_v, w_o, w_gate, w_up, w_down, norm_gain, qk_gain):
        rows, width = hidden.shape
        dim = qk_gain.shape[-1]
        n_kv = w_k.shape[-1] // dim
        angles = [angles_of(positions, dim, theta) for theta in THETAS]
        cuts = (96, 48)
        o_0, k_cache, v_cache, wo_0 = first_call(n_tp, n_cp, hidden, w_q, w_k, w_v, w_o, norm_gain, qk_gain, *angles[0])
        following = [w_q, w_k, w_v, qk_gain, *angles[1], k_cache, v_cache]
        x_1, _, q_1, k_all, vt_all, k_cache, v_cache, wo_1 = block_call(0, n_tp, n_cp, *cuts, o_0, w_o, wo_0, hidden, w_gate, w_up, w_down, norm_gain, following=following)
        o_1, gathered, wo_1 = global_call(n_tp, n_cp, *cuts, q_1, k_all, vt_all, w_o, wo_1, dim)
        x_2, _ = block_call(1, n_tp, n_cp, *cuts, o_1, w_o, wo_1, x_1, w_gate, w_up, w_down, norm_gain, gathered=gathered)
        return x_2, k_cache, v_cache

    return jax.shard_map(
        device_fn,
        mesh=mesh,
        in_specs=(row_spec, P(('dp', 'cp')), col_spec, col_spec, col_spec, row_w_spec, col_spec, col_spec, row_w_spec, P(), P()),
        out_specs=(row_spec, cache_spec, cache_spec),
        check_vma=False,
    )
```

```python
import functools
import types
import jax
import jax.numpy as jnp
from jax import lax
from jax.experimental import pallas as pl
from jax.experimental.pallas import tpu as pltpu
from jax.sharding import PartitionSpec as P

WINDOW = 1024
THETAS = (10000.0, 1000000.0)
EPS = 1e-6
NEG_BIG = -1e30
BF = jnp.bfloat16
F32 = jnp.float32
MESH = pl.DeviceIdType.MESH
ANY = pl.BlockSpec(memory_space=pl.ANY)
LOG2E = 1.4426950408889634
PAIR = 2
TWO = (0, 1)
TRIO = (0, 1, 2)
TILE = 256
LANES = 128
BIG_VMEM = 67_000_000
DMA = pltpu.SemaphoreType.DMA
VM = pltpu.VMEM
GATHER_SEMS = [DMA((3, PAIR))] * 8 + [DMA((6, 3))] * PAIR


def span(start, size, unit=16):
    return pl.ds(pl.multiple_of(start, unit), size)


def send(src, dst, sent, received, to):
    return pltpu.make_async_remote_copy(src_ref=src, dst_ref=dst, send_sem=sent, recv_sem=received, device_id=to, device_id_type=MESH)


def each(method, *groups):
    for group in groups:
        for item in group:
            getattr(item, method)()


def start(*groups):
    each('start', *groups)


def wait(*groups):
    each('wait', *groups)


def arrived(*groups):
    each('wait_recv', *groups)


def departed(*groups):
    each('wait_send', *groups)


def greet(peers):
    barrier = pltpu.get_barrier_semaphore()
    for to in peers:
        pl.semaphore_signal(barrier, inc=1, device_id=to, device_id_type=MESH)
    pl.semaphore_wait(barrier, len(peers))


def gain_of(ref, layer, row):
    return 1.0 + ref[layer, row:row + 1, :]


def around(axis, n, *distances):
    return [lax.rem(lax.axis_index(axis) + n + d, n) for d in distances]


def tp_peers(n_tp):
    return around('tp', n_tp, 1, -1, PAIR)


def cp_peers(n_cp):
    cp = lax.axis_index('cp')
    return (*around('cp', n_cp, PAIR, -PAIR, PAIR * PAIR), cp + 1 - PAIR * lax.rem(cp, PAIR))


def head_of(size):
    return pl.ds(0, size)


def on(axis, *devices):
    return [{axis: dev} for dev in devices]


def mean_scale(values):
    return lax.rsqrt(jnp.mean(values * values, axis=-1, keepdims=True) + EPS)


def rotate_heads(values, gain, cosine, sine):
    half = cosine.shape[-1]
    normed = values * mean_scale(values) * gain
    lower, upper = normed[:, :half], normed[:, half:]
    return jnp.concatenate([lower * cosine - upper * sine, upper * cosine + lower * sine], axis=-1).astype(BF)


def weight_gather(n_tp, n_cp, strip, cut, shard, whole, y1s, y1r, y2s, y2r, x1s=None, x1r=None, x2s=None, x2r=None, rs=None, rr=None):
    n_x = n_cp // PAIR
    half = whole.shape[1] // PAIR
    shared = (half - n_x * strip) // PAIR
    me, cp = lax.axis_index('tp'), lax.axis_index('cp')
    chip, base = cp // PAIR, lax.rem(cp, PAIR) * half
    right, left, opposite = tp_peers(n_tp)
    sides, sources = on('tp', right, left), (left, right, opposite)
    *ends, _, partner = on('cp', *cp_peers(n_cp))

    def strip_of(distance):
        return base + PAIR * shared + lax.rem(chip + n_x + distance, n_x) * strip

    pieces = ((strip_of(0), strip, strip // PAIR), (base, shared, shared // PAIR), (base + shared, shared, shared // PAIR))
    count = len(pieces)

    def halves(first, size, cut):
        return span(first, cut), span(first + cut, size - cut)

    def y_first(p):
        at = span(*pieces[p][:PAIR])
        return [send(shard.at[at, :], whole.at[me, at, :], y1s.at[p, d], y1r.at[p, d], sides[d]) for d in TWO]

    def y_second(p):
        refs = [whole.at[sources[d], halves(*pieces[p])[d], :] for d in TWO]
        return [send(refs[d], refs[d], y2s.at[p, d], y2r.at[p, d], sides[d]) for d in TWO]

    def x_first(s):
        ref = whole.at[sources[s], span(strip_of(0), strip), :]
        return [send(ref, ref, x1s.at[s, d], x1r.at[s, d], ends[d]) for d in TWO]

    def x_second(s):
        refs = [whole.at[sources[s], halves(strip_of((-1, 1)[d]), strip, cut)[d], :] for d in TWO]
        return [send(refs[d], refs[d], x2s.at[s, d], x2r.at[s, d], ends[d]) for d in TWO]

    def relay(kind, s):
        first, size = pieces[kind][:PAIR] if kind < count else (strip_of(kind + 1 - count), strip)
        ref = whole.at[sources[s], span(first, size), :]
        return [send(ref, ref, rs.at[kind, s], rr.at[kind, s], partner)]

    def y_stage(p, *more):
        arrived(y_first(p))
        start(y_second(p), *more, *[relay(p, s) for s in TWO])

    def y_end(p):
        arrived(y_second(p))
        start(relay(p, PAIR))

    def x_stage(s):
        arrived(x_first(s))
        start(x_second(s), relay(count, s), relay(count + PAIR, s))

    def x_end(s):
        arrived(x_second(s))
        start(relay(count + 1, s))

    def drain(parts):
        for s in TRIO:
            wait(*[relay(kind, s) for kind in range(PAIR * count)])
            departed(x_first(s), x_second(s))
        for p in parts:
            departed(y_first(p), y_second(p))

    peers = (*sides, *ends, partner)
    return types.SimpleNamespace(**{f.__name__: f for f in (y_first, y_second, x_first, x_second, relay, y_stage, y_end, x_stage, x_end, drain)}, peers=peers)


def keep_heads(rows_ref, out_ref):
    dim = out_ref.shape[-1]

    @pl.loop(0, out_ref.shape[1] // LANES)
    def _(i):
        at = span(i * LANES, LANES)
        for t in TWO:
            out_ref[t, at] = jnp.stack([rows_ref[t, at, begin:begin + dim] for begin in range(0, rows_ref.shape[-1], dim)], axis=1)


def first_kernel(
    n_q, n_kv, n_tp, n_cp, strip, cut,
    x_ref, wk_ref, wv_ref, wq_ref, gain_ref, hg_ref, cos_ref, sin_ref, wo_hbm,
    o_hbm, kc_hbm, vc_hbm, wo_all,
    h_ref, q_ref, kv_ref, past_ref, cache_ref,
    ks, kr, csem, osem, *sems,
):
    step = pl.program_id(0)
    rows = x_ref.shape[0]
    dim = hg_ref.shape[-1]
    g = weight_gather(n_tp, n_cp, strip, cut, wo_hbm.at[0], wo_all, *sems)
    follow, prior = on('cp', *around('cp', n_cp, 1, -1))

    def send_kv(t):
        return [send(kv_ref.at[t], past_ref.at[t], ks.at[t], kr.at[t], follow)]

    def keep_kv(t):
        return [pltpu.make_async_copy(cache_ref.at[t], (kc_hbm, vc_hbm)[t].at[0], csem.at[t])]

    group = n_q // n_kv

    keep_o = [pltpu.make_async_copy(q_ref, o_hbm, osem)]

    q_step = PAIR * n_kv

    @pl.when(step == 0)
    def _():
        greet((*g.peers[:-1], follow, prior))
        start(*map(g.y_first, TWO))
        rb = 32

        @pl.loop(0, rows // rb)
        def _(i):
            at = span(i * rb, rb)
            xf = x_ref[at, :].astype(F32)
            h_ref[at, :] = (xf * mean_scale(xf) * gain_of(gain_ref, 0, 0)).astype(BF)

    @pl.when(step == n_kv)
    def _():
        start(send_kv(0))

    @pl.when(step == q_step)
    def _():
        g.y_stage(0, g.y_first(PAIR), *map(g.x_first, TWO))
        start(send_kv(1))

    def project(w_ref, store, finish):
        @pl.loop(0, rows // TILE)
        def _(i):
            at = span(i * TILE, TILE)
            store(at, finish(jnp.dot(h_ref[at, :], w_ref[0], preferred_element_type=F32), at))

    def into_kv(t, head):
        def store(at, value):
            kv_ref[t, at, span(head * dim, dim, LANES)] = value
        return store

    def into_q(at, value):
        q_ref[at, span((step - q_step) * dim, dim, LANES)] = value

    def rotate(row):
        return lambda a, at: rotate_heads(a, gain_of(hg_ref, 0, row), cos_ref[at, :], sin_ref[at, :])

    @pl.when(step < n_kv)
    def _():
        project(wk_ref, into_kv(0, step), rotate(1))

    @pl.when((step >= n_kv) & (step < q_step))
    def _():
        project(wv_ref, into_kv(1, step - n_kv), lambda a, at: a.astype(BF))

    @pl.when(step >= q_step)
    def _():
        project(wq_ref, into_q, rotate(0))

    @pl.when(step == q_step + n_q - 1)
    def _():
        keep_heads(kv_ref, cache_ref)
        start(*map(keep_kv, TWO))
        g.y_stage(1)
        g.y_end(0)
        start(g.x_first(PAIR))
        g.x_stage(0)
        g.x_stage(1)
        g.y_stage(PAIR)
        arrived(*map(send_kv, TWO))

        @pl.loop(0, n_kv)
        def _(h):
            head = span(h * dim, dim, LANES)

            @pl.loop(0, group)
            def _(i):
                local_head(q_ref, h * group + i, *[ref.at[t, :, head] for t in TWO for ref in (past_ref, kv_ref)])

            @pl.when(h == 0)
            def _():
                g.x_end(0)
                g.x_stage(PAIR)

        start(keep_o)
        g.x_end(1)
        g.y_end(1)
        g.y_end(PAIR)
        g.x_end(PAIR)
        departed(*map(send_kv, TWO))
        wait(*map(keep_kv, TWO), keep_o)
        g.drain(TRIO)


def first_call(n_tp, n_cp, x, w_q, w_k, w_v, w_o, gain, head_gain, cosine, sine):
    rows, width = x.shape
    dim = head_gain.shape[-1]
    n_q, n_kv = w_q.shape[-1] // dim, w_k.shape[-1] // dim
    at_k = lambda t: jnp.minimum(t, n_kv - 1)
    at_v = lambda t: jnp.clip(t - n_kv, 0, n_kv - 1)
    at_q = lambda t: jnp.maximum(t - PAIR * n_kv, 0)
    whole = lambda a: pl.BlockSpec(a.shape, lambda t: TWO[:1] * a.ndim, pipeline_mode=pl.Buffered(1))
    w_spec = lambda at: pl.BlockSpec((1, width, dim), lambda t: (0, 0, at(t)))
    shape = lambda *sizes: jax.ShapeDtypeStruct(sizes, BF)
    q_width, kv_width = n_q * dim, n_kv * dim
    work = PAIR * width * (q_width + PAIR * kv_width)
    gathered, cache = shape(n_tp, *w_o.shape[1:]), shape(PAIR, rows, n_kv, dim)
    flat = (PAIR, rows, kv_width)
    return pl.pallas_call(
        functools.partial(first_kernel, n_q, n_kv, n_tp, n_cp, 64, 16),
        grid=(n_q + PAIR * n_kv,),
        in_specs=[whole(x), *map(w_spec, (at_k, at_v, at_q)), *map(whole, (gain, head_gain, cosine, sine)), ANY],
        out_specs=[ANY] * 4,
        out_shape=[shape(rows, q_width), cache, cache, gathered],
        scratch_shapes=[VM((rows, width), BF), VM((rows, q_width), BF), VM(flat, BF), VM(flat, BF), VM(cache.shape, BF)]
        + [DMA((PAIR,))] * 3 + [DMA] + GATHER_SEMS,
        compiler_params=pltpu.CompilerParams(dimension_semantics=("arbitrary",), collective_id=2, has_side_effects=True, vmem_limit_bytes=BIG_VMEM),
        cost_estimate=pl.CostEstimate(flops=rows * work, bytes_accessed=work, transcendentals=0),
        name="first",
    )(x, w_k, w_v, w_q, gain, head_gain, cosine, sine, w_o)


def scores_of(q, k):
    return lax.dot_general(q, k, (((1,), (1,)), ((), ())), preferred_element_type=F32)


def local_head(q_ref, head, kp_ref, ko_ref, vp_ref, vo_ref):
    rows, dim = ko_ref.shape
    tile = TILE
    scale = dim ** -0.5 * LOG2E
    opening = lax.axis_index('cp') == 0
    row = lax.broadcasted_iota(jnp.int32, (tile, tile), 0)
    col = lax.broadcasted_iota(jnp.int32, (tile, tile), 1)
    for begin in range(0, rows, tile):
        end = begin + tile
        at = (slice(begin, end), span(head * dim, dim, LANES))
        q = q_ref[at]
        past = scores_of(q, kp_ref[begin:, :])
        here = scores_of(q, ko_ref[:end, :])
        past = jnp.concatenate([jnp.where(col > row, past[:, :tile], NEG_BIG), past[:, tile:]][:1 + (end < rows)], axis=1)
        past = jnp.where(opening, NEG_BIG, past)
        here = jnp.concatenate([here[:, :begin], jnp.where(col <= row, here[:, begin:], NEG_BIG)][begin == 0:], axis=1)
        top = jnp.maximum(*[jnp.max(a, axis=1, keepdims=True) for a in (past, here)])
        probs = [jnp.exp2((a - top) * scale) for a in (past, here)]
        total = sum(jnp.sum(p, axis=1, keepdims=True) for p in probs)
        acc = sum(jnp.dot(p.astype(BF), v, preferred_element_type=F32) for p, v in zip(probs, (vp_ref[begin:, :], vo_ref[:end, :])))
        q_ref[at] = (acc / total).astype(BF)


def fold_rows(values, op):
    return op(values.reshape(-1, 8, values.shape[-1]), axis=0)


def row_gather(n_tp, unit, gathered, own, s1, r1, s2, r2):
    sides = on('tp', *tp_peers(n_tp)[:PAIR])
    half = gathered.shape[-1] // PAIR
    seen = TRIO[::-PAIR]

    def first(u):
        at = span(u * unit, unit)
        return [send(own.at[at, :], gathered.at[seen[d], at, :], s1.at[u, d], r1.at[u, d], sides[d]) for d in TWO]

    def second(u):
        at = span(u * unit, unit)
        cols = [slice(d * half, (d + 1) * half) for d in TWO]
        return [send(gathered.at[seen[d], at, cols[d]], gathered.at[1, at, cols[d]], s2.at[u, d], r2.at[u, d], sides[d]) for d in TWO]

    return sides, first, second


def global_kernel(
    groups, n_tp, n_cp, unit, strip, cut, q_ref, k_hbm, vt_hbm, wo_hbm, _, o_hbm, og_hbm, wn_hbm,
    k_ref, vt_ref, o_ref, m_ref, l_ref, ka_ref, kb_ref, xa_ref, xb_ref, acc_ref, sa_ref, sb_ref, pa_ref, pb_ref,
    ksem, vsem, osem, s1, r1, s2, r2, *sems,
):
    rows, width = q_ref.shape
    dim = acc_ref.shape[0]
    n_kv = k_hbm.shape[1] // dim
    block, wide = sa_ref.shape
    tile = wide // groups
    scale = dim ** -0.5 * LOG2E
    cp = lax.axis_index('cp')
    base = cp * (rows // block)
    last = base - 1
    _, first, second = row_gather(n_tp, unit, og_hbm, o_ref, s1, r1, s2, r2)
    w = weight_gather(n_tp, n_cp, strip, cut, wo_hbm.at[1], wn_hbm, *sems)
    ready = tile // unit

    def load(b):
        at = span(b * rows, rows, LANES)
        return [pltpu.make_async_copy(k_hbm.at[at, :], k_ref.at[at, :], ksem.at[b]), pltpu.make_async_copy(vt_hbm.at[:, at], vt_ref.at[:, at], vsem.at[b])]

    def store(i):
        at = span(i * tile, tile)
        return [pltpu.make_async_copy(o_ref.at[at, :], o_hbm.at[at, :], osem.at[i])]

    start(load(cp))

    @pl.loop(0, cp)
    def _(b):
        start(load(b))

    greet(w.peers)
    start(w.y_first(1), w.y_first(PAIR), *map(w.x_first, TRIO), *[w.relay(0, s) for s in TRIO])
    wait(load(cp))

    key = lax.broadcasted_iota(jnp.int32, (block, wide), 0)
    token = lax.rem(lax.broadcasted_iota(jnp.int32, (block, wide), 1), tile)

    @pl.loop(0, n_kv * (rows // tile))
    def _(turn):
        i, h = turn // n_kv, lax.rem(turn, n_kv)
        head = span(h * dim, dim, LANES)

        q = jnp.concatenate([q_ref[span(i * tile, tile), span((h * groups + g) * dim, dim, LANES)] for g in range(groups)], axis=0)

        def score(b, s_ref, x_ref, masked=False):
            s = scores_of(k_ref[span(b * block, block), head], q)
            if masked:
                s = jnp.where(key <= token, s, NEG_BIG)
            s_ref[...] = s
            x_ref[...] = fold_rows(s, jnp.max)

        def soften(s_ref, x_ref, p_ref, keep_ref, opening=False):
            top = jnp.max(x_ref[...], axis=0, keepdims=True)
            if not opening:
                old = m_ref[...]
                top = jnp.maximum(old, top)
                keep_ref[...] = jnp.exp2((old - top) * scale)
            m_ref[...] = top
            prob = jnp.exp2((s_ref[...] - top) * scale)
            part = fold_rows(prob, jnp.sum)
            l_ref[...] = part if opening else l_ref[...] * keep_ref[...] + part
            p_ref[...] = prob.astype(BF)

        def weigh(b, p_ref, keep_ref, opening=False):
            part = jnp.dot(vt_ref[head, span(b * block, block, LANES)], p_ref[...], preferred_element_type=F32)
            acc_ref[...] = part if opening else acc_ref[...] * keep_ref[...] + part

        score(base + i, sa_ref, xa_ref, True)
        soften(sa_ref, xa_ref, pa_ref, ka_ref, True)
        weigh(base + i, pa_ref, ka_ref, True)

        @pl.loop(0, i)
        def _(b):
            score(base + b, sa_ref, xa_ref)
            soften(sa_ref, xa_ref, pa_ref, ka_ref)
            weigh(base + b, pa_ref, ka_ref)

        def loaded(b):
            @pl.when((turn == 0) & (b < cp))
            def _():
                wait(load(b))

        @pl.when(cp > 0)
        def _():
            loaded(0)
            score(jnp.int32(0), sa_ref, xa_ref)
            pb_ref[...] = jnp.zeros_like(pb_ref)
            kb_ref[...] = jnp.ones_like(kb_ref)

            @pl.loop(0, base // PAIR)
            def _(half):
                b = PAIR * half
                loaded(half + 1)
                score(b + 1, sb_ref, xb_ref)
                soften(sa_ref, xa_ref, pa_ref, ka_ref)
                weigh(jnp.maximum(b - 1, 0), pb_ref, kb_ref)
                score(jnp.minimum(b + PAIR, last), sa_ref, xa_ref)
                soften(sb_ref, xb_ref, pb_ref, kb_ref)
                weigh(b, pa_ref, ka_ref)

            weigh(last, pb_ref, kb_ref)

        out = (acc_ref[...] / jnp.sum(l_ref[...], axis=0, keepdims=True)).T.astype(BF)
        for g in range(groups):
            o_ref[span(i * tile, tile), span((h * groups + g) * dim, dim, LANES)] = out[g * tile:(g + 1) * tile]

        @pl.when(turn == 0)
        def _():
            w.y_stage(1)
            w.x_stage(0)

        @pl.when(turn == n_kv - 1)
        def _():
            start(store(0), *map(first, range(ready)))
            w.y_stage(PAIR)
            w.x_stage(1)

        @pl.when(turn == n_kv)
        def _():
            w.x_stage(PAIR)
            w.y_end(1)
            for u in range(ready - 1):
                arrived(first(u))
                start(second(u))

    start(store(1))
    arrived(first(ready - 1))
    start(second(ready - 1))
    w.x_end(0)
    w.x_end(1)
    w.y_end(PAIR)
    w.x_end(PAIR)
    for u in range(ready):
        departed(first(u))
        wait(second(u))
    wait(*map(store, TWO))
    w.drain(TRIO[1:])


def global_call(n_tp, n_cp, strip, cut, q, k_all, vt_all, w_o, wo_next, dim):
    rows, width = q.shape
    every, kv_width = k_all.shape
    groups = width // kv_width
    tile = rows // PAIR
    wide = groups * tile
    unit = LANES
    vmem = pl.BlockSpec(memory_space=VM)
    row, slab = VM((1, wide), F32), VM((8, wide), F32)
    return pl.pallas_call(
        functools.partial(global_kernel, groups, n_tp, n_cp, unit, strip, cut),
        in_specs=[vmem] + [ANY] * 4,
        out_specs=[ANY] * 3,
        out_shape=[jax.ShapeDtypeStruct(size, BF) for size in (q.shape, (n_tp - 1, *q.shape), wo_next.shape)],
        input_output_aliases={4: PAIR},
        scratch_shapes=[VM(k_all.shape, BF), VM(vt_all.shape, BF), VM(q.shape, BF), row, slab, row, row, slab, slab, VM((dim, wide), F32)]
        + [VM((tile, wide), t) for t in (F32, F32, BF, BF)] + [DMA((every // rows,))] * PAIR + [DMA((PAIR,))] + [DMA((tile // unit, PAIR))] * 4 + GATHER_SEMS,
        compiler_params=pltpu.CompilerParams(collective_id=3, has_side_effects=True, vmem_limit_bytes=BIG_VMEM),
        cost_estimate=pl.CostEstimate(flops=PAIR * rows * every * width, bytes_accessed=PAIR * every * width, transcendentals=0),
        name="attend_global",
    )(q, k_all, vt_all, w_o, wo_next)


def block_kernel(layer, n_tp, n_cp, tm, nt, unit, strip, cut, ready, follow, *refs):
    queue = iter(refs)

    def take(names):
        return [ref for _, ref in zip(range(names), queue)]

    o_hbm, wo_own, wo_hbm, x_hbm, wg_hbm, wu_hbm, wd_hbm, gain_ref = take(8)
    if ready:
        take(1)
    if follow:
        wq_hbm, wk_hbm, wv_hbm, hg_ref, cos_ref, sin_ref, *_ = take(8)
    out_hbm, og_hbm = take(PAIR)
    if follow:
        q_hbm, ka_hbm, va_hbm, k_hbm, v_hbm, wn_hbm = take(6)
    wbuf, pbuf, r1, r2, xb, mbuf, sbuf, gbuf, obuf, xbuf, rown, wsem, osem, xsem, stsem = take(15)
    o1s, o1r, o2s, o2r, s1s, s1r, sbs, sbr, sas, sar, g1s, g1r, g2s, g2r = take(14)
    if follow:
        nbuf, vbuf, cbuf, nsem, fs, fr, hs, hr, ps, pr, *sems = take(14)
        w = weight_gather(n_tp, n_cp, strip, cut, wo_own.at[layer + 1], wn_hbm, *sems)

    rows, width = x_hbm.shape
    o_width = o_hbm.shape[1]
    hidden = wd_hbm.shape[1]
    chunks = rows // tm
    fine = tm // unit
    br = unit // n_tp
    hw = width // PAIR
    units = rows // unit
    n_o, n_g, n_d = width // nt, hidden // nt, width // nt
    n_og = n_o + PAIR * n_g
    per = n_og + n_d
    depth, lag = 3, PAIR
    n_n = 0
    if follow:
        dim = hg_ref.shape[-1]
        nw = wk_hbm.shape[-1]
        n_qt = wq_hbm.shape[-1] // nw
        n_n = n_qt + PAIR
    total = chunks * per + (chunks + 1) * n_n

    me, cp = lax.axis_index('tp'), lax.axis_index('cp')
    right, left, opposite = tp_peers(n_tp)
    near = (right, left)
    far = (left, right)
    ahead, behind, across, mate = cp_peers(n_cp)
    *ends, partner = on('cp', ahead, behind, mate)
    sides, o_first, o_second = row_gather(n_tp, unit, og_hbm, o_hbm, o1s, o1r, o2s, o2r)

    def base_of(n):
        return n * per + jnp.maximum(n - lag, 0) * n_n

    def step_of(index):
        if not follow:
            return lax.rem(index, per)
        head, body = lag * per, (chunks - lag) * (per + n_n)
        late = index - head
        tail = per + lax.rem(jnp.maximum(late - body, 0), n_n)
        return jnp.where(late < 0, lax.rem(index, per), jnp.where(late < body, lax.rem(jnp.maximum(late, 0), per + n_n), tail))

    def columns(tile):
        return span(tile * nt, nt, LANES)

    def part_of(slot, length, first=0):
        return wbuf.at[slot, pl.ds(first, length), :]

    def narrow(slot):
        return wbuf.at[slot, head_of(width), head_of(nw)]

    def start_w(index):
        step, slot = step_of(index), lax.rem(index, depth)

        def load(wanted, src, dst, s=0):
            @pl.when((index < total) & wanted)
            def _():
                pltpu.make_async_copy(src, dst, wsem.at[slot, s]).start()

        for s in range(n_tp):
            src = wo_hbm.at[lax.rem(me + s, n_tp)] if s else wo_own.at[layer]
            load(step < n_o, src.at[:, columns(jnp.minimum(step, n_o - 1))], part_of(slot, o_width, s * o_width), s)
        middle = jnp.clip(step - n_o, 0, n_og - n_o - 1)
        for t, src in enumerate((wg_hbm, wu_hbm)):
            load((step >= n_o) & (step < n_og) & (lax.rem(middle, PAIR) == t), src.at[layer, :, columns(middle // PAIR)], part_of(slot, width))
        load((step >= n_og) & (step < per), wd_hbm.at[layer, :, columns(jnp.clip(step - n_og, 0, n_d - 1))], part_of(slot, hidden))
        if follow:
            for t, src in enumerate((wk_hbm, wv_hbm)):
                load(step == per + t, src.at[layer + 1], narrow(slot))
            late = step - per - PAIR
            load(late >= 0, wq_hbm.at[layer + 1, :, span(jnp.clip(late, 0, n_qt - 1) * nw, nw, LANES)], narrow(slot))

    def wait_w(index, length):
        slot = lax.rem(index, depth)
        pltpu.make_async_copy(wd_hbm.at[layer, head_of(length), columns(0)], part_of(slot, length), wsem.at[slot, 0]).wait()
        return slot

    def wait_wo(index):
        slot = lax.rem(index, depth)
        for s in range(n_tp):
            pltpu.make_async_copy(wo_own.at[layer, :, columns(0)], part_of(slot, o_width, s * o_width), wsem.at[slot, s]).wait()
        return slot

    def o_serve(u):
        arrived(o_first(u))
        start(o_second(u))

        @pl.when(u + PAIR < units)
        def _():
            start(o_first(u + PAIR))

    def o_finish(u):
        departed(o_first(u))
        wait(o_second(u))

    cols = [pl.ds(d * hw, hw) for d in TWO]
    other = cols[::-1]

    def partial(k):
        return pbuf.at[lax.rem(k // fine, PAIR)]

    def part(k, dev):
        return span(lax.rem(k, fine) * unit + dev * br, br)

    def reduce(kind, k, d, dev, side, dst):
        s_sem, r_sem = kind
        return [send(partial(k).at[part(k, dev), side], dst, s_sem.at[k, d], r_sem.at[k, d], sides[d])]

    def s_far(k, d):
        return reduce((s1s, s1r), k, d, opposite, cols[d], r1.at[k, d])

    def s_plain(k, d):
        return reduce((sbs, sbr), k, d, near[d], other[d], r2.at[k, d, :, other[d]])

    def s_sum(k, d):
        return reduce((sas, sar), k, d, near[d], cols[d], r2.at[k, d, :, cols[d]])

    def x_rows(k, dev):
        return span(k * unit + dev * br, br)

    def x_first(k):
        return [send(xb.at[k], out_hbm.at[x_rows(k, me), :], g1s.at[k, d], g1r.at[k, d], sides[d]) for d in TWO]

    def x_second(k):
        refs = [out_hbm.at[x_rows(k, far[d]), cols[d]] for d in TWO]
        return [send(refs[d], refs[d], g2s.at[k, d], g2r.at[k, d], sides[d]) for d in TWO]

    def x_own(k):
        return [pltpu.make_async_copy(xb.at[k], out_hbm.at[x_rows(k, me), :], stsem.at[k])]

    def e0(n):
        for kind in (s_far, s_plain):
            for i in range(fine):
                start(*[kind(n * fine + i, d) for d in TWO])

    def e1(k):
        p = partial(k)
        for d in TWO:
            at = (part(k, near[d]), cols[d])
            arrived(s_far(k, d))
            p[at] = p[at] + r1[k, d]
            start(s_sum(k, d))

    def e2(k):
        p = partial(k)
        for d in TWO:
            arrived(s_plain(k, d), s_sum(k, d))
        sub = 16
        for begin in range(0, br, sub):
            at = pl.ds(begin, sub)
            z = sum([r2[k, d, at, :] for d in TWO], p[span(lax.rem(k, fine) * unit + me * br + begin, sub), :])
            r = rown[lax.rem(k // fine, PAIR), lax.rem(k, fine), at, :].astype(F32)
            xb[k, at, :] = (r + z * mean_scale(z) * gain_of(gain_ref, layer, 3)).astype(BF)
        start(x_first(k), x_own(k))
        for d in TWO:
            departed(s_far(k, d), s_plain(k, d), s_sum(k, d))

    def e3(k):
        arrived(x_first(k))
        start(x_second(k))

    def e4(k):
        wait(x_second(k), x_own(k))
        departed(x_first(k))

    def all_of(step, n):
        for i in range(fine):
            step(n * fine + i)

    def batch(n):
        return n, n * tm, tm

    ends_of = [(jnp.int32(chunks - 1 + i), jnp.int32(rows - tm + i * unit), unit) for i in TWO]

    def kv_at(c, dev, t):
        at = span(dev * rows + c[1], c[PAIR], LANES)
        return va_hbm.at[:, at] if t else ka_hbm.at[at, :]

    def kv_mine(c, t):
        slot, some = lax.rem(c[0], depth), head_of(c[PAIR])
        return vbuf.at[slot, :, some] if t else nbuf.at[slot, 0, some, :]

    def kv_first(c):
        return [send(kv_mine(c, t), kv_at(c, cp, t), fs.at[c[0], t, d], fr.at[c[0], t, d], to) for t in TWO for d, to in enumerate((*ends, partner))]

    def kv_second(c):
        refs = [kv_at(c, (behind, ahead)[d], d) for d in TWO]
        return [send(refs[d], refs[d], hs.at[c[0], d], hr.at[c[0], d], ends[d]) for d in TWO]

    def kv_relay(c, e):
        refs = [kv_at(c, (behind, ahead, across)[e], t) for t in TWO]
        return [send(refs[t], refs[t], ps.at[c[0], e, t], pr.at[c[0], e, t], partner) for t in TWO]

    def stores(c):
        k, first, size = c
        at, slot, some = span(first, size), lax.rem(k, depth), head_of(size)
        pairs = [(kv_mine(c, t), kv_at(c, cp, t)) for t in TWO] + [(cbuf.at[slot, t, some], (k_hbm, v_hbm)[t].at[1, at]) for t in TWO]
        pairs += [(nbuf.at[slot, PAIR + t, some, :], q_hbm.at[at, pl.ds(t * nw, nw)]) for t in range(n_qt)]
        return [pltpu.make_async_copy(src, dst, nsem.at[slot, t]) for t, (src, dst) in enumerate(pairs)]

    def f0(c, base):
        k, first, size = c
        at, slot, some = span(first, size), lax.rem(k, depth), head_of(size)
        load = [pltpu.make_async_copy(out_hbm.at[at, :], xbuf.at[some, :], xsem)]
        start(load)
        wait(load)
        sub = 32

        @pl.loop(0, size // sub)
        def _(i):
            rows_of = span(i * sub, sub)
            xf = xbuf[rows_of, :].astype(F32)
            mbuf[rows_of, :] = (xf * mean_scale(xf) * gain_of(gain_ref, layer + 1, 0)).astype(BF)

        cosine, sine = cos_ref[at, :], sin_ref[at, :]

        def project(t, finish):
            start_w(base + t + PAIR)
            w_slot = lax.rem(base + t, depth)
            pltpu.make_async_copy(wk_hbm.at[layer + 1], narrow(w_slot), wsem.at[w_slot, 0]).wait()

            @pl.loop(0, nw // dim)
            def _(h):
                this = span(h * dim, dim, LANES)
                finish(this, jnp.dot(mbuf[some, :], wbuf[w_slot, head_of(width), this], preferred_element_type=F32))

        def rotate(t, row):
            def finish(this, acc):
                nbuf[slot, t, some, this] = rotate_heads(acc, gain_of(hg_ref, layer + 1, row), cosine, sine)
            return finish

        def plain(this, acc):
            nbuf[slot, 1, some, this] = acc.astype(BF)
            vbuf[slot, this, some] = acc.T.astype(BF)

        project(0, rotate(0, 1))
        project(1, plain)
        start(kv_first(c))

        @pl.loop(PAIR, n_n)
        def _(t):
            project(t, rotate(t, 0))

        keep_heads(nbuf.at[slot, :, some], cbuf.at[slot, :, some])
        start(stores(c))

    def f1(c):
        arrived(kv_first(c))
        start(kv_second(c), *[kv_relay(c, e) for e in TWO])

    def f2(c):
        arrived(kv_second(c))
        start(kv_relay(c, PAIR))
        departed(kv_first(c))
        wait(stores(c))

    def f3(c):
        wait(*[kv_relay(c, e) for e in TRIO])
        departed(kv_second(c))

    for t in TWO:
        start_w(jnp.int32(t))
    greet((*sides, *ends, partner) if follow else sides)
    start(*[o_first(ready + t) for t in TWO])
    served = ready
    if not ready:
        for served in TWO:
            arrived(o_first(served))
            start(o_second(served))
        served = PAIR
        start(*[o_first(served + t) for t in TWO])

    def serve(n, place):
        if served + place < units:
            @pl.when(n == 0)
            def _():
                o_serve(served + place)

    def load_rows(n):
        at = span(n * tm, tm)
        copies = [pltpu.make_async_copy(x_hbm.at[at, :], xbuf, xsem)]
        for s in range(n_tp):
            src = og_hbm.at[s - 1] if s else o_hbm
            copies.append(pltpu.make_async_copy(src.at[at, :], obuf.at[:, pl.ds(s * o_width, o_width)], osem.at[s]))
        return copies

    def between(n, j):
        @pl.when((j == 0) & (n >= 1))
        def _():
            all_of(e1, n - 1)

        @pl.when(j == 1)
        def _():
            serve(n, PAIR)

            @pl.when(n >= lag)
            def _():
                all_of(e3, n - lag)

        @pl.when(j == depth)
        def _():
            serve(n, depth)

    def chunk(n, _):
        base = base_of(n)
        slot_p = lax.rem(n, PAIR)
        p = pbuf.at[slot_p]

        @pl.when(n * tm >= ready * unit)
        def _():
            all_of(o_finish, n)

        start(load_rows(n))
        wait(load_rows(n))

        @pl.loop(0, n_o)
        def _(j):
            start_w(base + j + PAIR)
            slot = wait_wo(base + j)
            p[:, columns(j)] = jnp.dot(obuf[...], wbuf[slot], preferred_element_type=F32)

            @pl.when(j == n_o // PAIR)
            def _():
                serve(n, 0)

        serve(n, 1)

        if follow:
            @pl.when(n > lag)
            def _():
                f1(batch(n - 1 - lag))

        sub = 32

        @pl.loop(0, tm // sub)
        def _(i):
            at = span(i * sub, sub)
            z = p[at, :]
            r = (xbuf[at, :].astype(F32) + z * mean_scale(z) * gain_of(gain_ref, layer, 1)).astype(BF)
            xbuf[at, :] = r
            rf = r.astype(F32)
            mbuf[at, :] = (rf * mean_scale(rf) * gain_of(gain_ref, layer, PAIR)).astype(BF)

        for i in range(fine):
            rown[slot_p, i] = xbuf[span(i * unit + me * br, br), :]

        @pl.loop(0, PAIR * n_g)
        def _(t):
            index, j, odd = base + n_o + t, t // PAIR, lax.rem(t, PAIR)
            start_w(index + PAIR)
            slot = wait_w(index, width)
            gbuf[odd] = jnp.dot(mbuf[...], part_of(slot, width)[...], preferred_element_type=F32)

            @pl.when(odd == 1)
            def _():
                sbuf[:, columns(j)] = (jax.nn.gelu(gbuf[0], approximate=True) * gbuf[1]).astype(BF)
                between(n, j)

        @pl.when(n >= 1)
        def _():
            all_of(e2, n - 1)

        if follow:
            @pl.when(n > lag)
            def _():
                f2(batch(n - 1 - lag))

        @pl.loop(0, n_d)
        def _(j):
            index = base + n_og + j
            start_w(index + PAIR)
            slot = wait_w(index, hidden)
            p[:, columns(j)] = jnp.dot(sbuf[...], part_of(slot, hidden)[...], preferred_element_type=F32)

            @pl.when(j == 0)
            def _():
                serve(n, 4)

        serve(n, 5)
        e0(n)

        @pl.when(n >= lag)
        def _():
            all_of(e4, n - lag)
            if follow:
                f0(batch(n - lag), base + per)

        return 0

    lax.fori_loop(0, chunks, chunk, 0)
    every = [jnp.int32(k) for k in range(chunks)]
    tail = jnp.int32(total - depth * n_n)
    *_, before, last = every
    all_of(e1, last)
    all_of(e3, before)
    if follow:
        early, middle, *late = *map(batch, every[1:-1]), *ends_of
        f1(early)
    all_of(e2, last)
    all_of(e4, before)
    if follow:
        f2(early)
        f0(middle, tail)
    all_of(e3, last)
    if follow:
        start(w.y_first(0))

        @pl.loop(0, fine)
        def _(i):
            e4(last * fine + i)
            f0((chunks - 1 + i, rows - tm + i * unit, unit), tail + (1 + i) * n_n)
            for t, step in enumerate((f1, f2)):
                @pl.when(i == t)
                def _():
                    step(middle)

        arrived(w.y_first(0))
        start(w.y_second(0))
        for step in (f1, f2):
            for c in late:
                step(c)
        arrived(w.y_second(0))
        departed(w.y_first(0), w.y_second(0))
        for c in (batch(every[0]), early, middle, *late):
            f3(c)
    else:
        all_of(e4, last)


def block_call(layer, n_tp, n_cp, strip, cut, o, w_o, wo_all, x, w_gate, w_up, w_down, gain, gathered=None, following=None):
    rows, width = x.shape
    o_width = o.shape[1]
    hidden = w_down.shape[1]
    tm, nt, unit = TILE, 768, LANES
    chunks, br, units = rows // tm, unit // n_tp, rows // unit
    vmem = pl.BlockSpec(memory_space=VM)
    deep = max(n_tp * o_width, width, hidden)
    shape = lambda *sizes: jax.ShapeDtypeStruct(sizes, BF)
    operands = [o, w_o, wo_all, x, w_gate, w_up, w_down, gain]
    in_specs = [ANY] * 7 + [vmem]
    out_shape = [shape(rows, width), shape(n_tp - 1, rows, o_width)]
    scratch = [
        VM((3, deep, nt), BF), VM((PAIR, tm, width), F32), VM((units, PAIR, br, width // PAIR), F32), VM((units, PAIR, br, width), F32),
        VM((units, br, width), BF), VM((tm, width), BF), VM((tm, hidden), BF), VM((PAIR, tm, nt), F32), VM((tm, n_tp * o_width), BF), VM((tm, width), BF), VM((PAIR, tm // unit, br, width), BF),
        DMA((3, n_tp)), DMA((n_tp,)), DMA, DMA((units,)),
    ] + [DMA((units, PAIR))] * 14
    aliases = {}
    if gathered is not None:
        aliases[len(operands)] = 1
        operands.append(gathered)
        in_specs.append(ANY)
    if following is not None:
        q_width, kv_width = following[0].shape[-1], following[1].shape[-1]
        n_qt = q_width // kv_width
        operands += following
        in_specs += [ANY] * 3 + [vmem] * 3 + [ANY] * PAIR
        kept = following[-PAIR:]
        out_shape += [shape(rows, q_width), shape(n_cp * rows, kv_width), shape(kv_width, n_cp * rows)] + [shape(*a.shape) for a in kept]
        aliases.update((len(operands) - i, len(out_shape) - i) for i in range(1, 1 + len(kept)))
        out_shape.append(shape(*wo_all.shape))
        scratch += [VM((3, n_qt + PAIR, tm, kv_width), BF), VM((3, kv_width, tm), BF), VM((3, PAIR, tm, *kept[0].shape[PAIR:]), BF), DMA((3, n_qt + 4))]
        late = chunks + 1
        for count, sizes in ((1, (late, PAIR, 3)), (1, (late, PAIR)), (1, (late, 3, PAIR)), (PAIR, (1, PAIR))):
            scratch += [DMA(sizes)] * (PAIR * count)
    weights = width * (n_tp * o_width + 3 * hidden)
    return pl.pallas_call(
        functools.partial(block_kernel, layer, n_tp, n_cp, tm, nt, unit, strip, cut, 0 if gathered is None else units // PAIR, following is not None),
        in_specs=in_specs,
        out_specs=[ANY] * len(out_shape),
        out_shape=out_shape,
        scratch_shapes=scratch,
        input_output_aliases=aliases,
        compiler_params=pltpu.CompilerParams(collective_id=layer, has_side_effects=True, vmem_limit_bytes=BIG_VMEM),
        cost_estimate=pl.CostEstimate(flops=4 * rows * weights, bytes_accessed=8 * weights, transcendentals=0),
        name=f"block_{layer}",
    )(*operands)


def angles_of(positions, dim, theta):
    inv_freq = theta ** (-(jnp.arange(dim // 2, dtype=F32) * 2.0) / dim)
    angles = positions.astype(F32)[..., None] * inv_freq
    return jnp.cos(angles), jnp.sin(angles)


def solution(mesh):
    n_cp, n_tp = mesh.shape['cp'], mesh.shape['tp']
    row_spec = P(('dp', 'cp'), None)
    col_spec = P(None, None, 'tp')
    row_w_spec = P(None, 'tp', None)
    cache_spec = P(None, ('dp', 'cp'), 'tp', None)

    def device_fn(hidden, positions, w_q, w_k, w_v, w_o, w_gate, w_up, w_down, norm_gain, qk_gain):
        rows, width = hidden.shape
        dim = qk_gain.shape[-1]
        n_kv = w_k.shape[-1] // dim
        angles = [angles_of(positions, dim, theta) for theta in THETAS]
        cuts = (96, 48)
        o_0, k_cache, v_cache, wo_0 = first_call(n_tp, n_cp, hidden, w_q, w_k, w_v, w_o, norm_gain, qk_gain, *angles[0])
        following = [w_q, w_k, w_v, qk_gain, *angles[1], k_cache, v_cache]
        x_1, _, q_1, k_all, vt_all, k_cache, v_cache, wo_1 = block_call(0, n_tp, n_cp, *cuts, o_0, w_o, wo_0, hidden, w_gate, w_up, w_down, norm_gain, following=following)
        o_1, gathered, wo_1 = global_call(n_tp, n_cp, *cuts, q_1, k_all, vt_all, w_o, wo_1, dim)
        x_2, _ = block_call(1, n_tp, n_cp, *cuts, o_1, w_o, wo_1, x_1, w_gate, w_up, w_down, norm_gain, gathered=gathered)
        return x_2, k_cache, v_cache

    return jax.shard_map(
        device_fn,
        mesh=mesh,
        in_specs=(row_spec, P(('dp', 'cp')), col_spec, col_spec, col_spec, row_w_spec, col_spec, col_spec, row_w_spec, P(), P()),
        out_specs=(row_spec, cache_spec, cache_spec),
        check_vma=False,
    )
```
